8 devices in a mesh: dp: 2 (over z, y), tp: 4 (over x, core).
Axes of the slice: x: 2, y: 2, z: 1, core: 2. Of those that a mesh axis runs over, the one named last changes fastest.
Arguments:
- hidden: bfloat16 [24, 1152, 2048], P('dp', 'tp'), parts along dimension 0
- prefix_len: int32 [24], P('dp'), parts along dimension 0
- valid_len: int32 [24], P('dp'), parts along dimension 0
- norm_attn: bfloat16 [2048], replicated
- w_query: bfloat16 [2048, 2048], P(None, 'tp')
- w_key: bfloat16 [2048, 256], replicated
- w_value: bfloat16 [2048, 256], replicated
- w_out: bfloat16 [2048, 2048], P('tp')
- norm_mlp: bfloat16 [2048], replicated
- w_gate: bfloat16 [2048, 16384], P(None, 'tp')
- w_up: bfloat16 [2048, 16384], P(None, 'tp')
- w_down: bfloat16 [16384, 2048], P('tp')
Outputs:
- output 1: bfloat16 [24, 1152, 2048], P('dp', 'tp'), parts along dimension 0
- output 2: bfloat16 [24, 1152, 256], P('dp', 'tp'), parts along dimension 0
- output 3: bfloat16 [24, 1152, 256], P('dp', 'tp'), parts along dimension 0
There are 2 independent parts. The reference program is written for one: setup_inputs(seed, part) draws one part's arguments, and reference() takes and returns one part's arrays. A program takes and returns all parts, laid end to end along the dimension named above; an argument that names none is the same for every part.
All inputs are finite; a program needn't handle non-finite values.
Results may differ from the reference program's by a relative error of at most 0.0131743.
Values are sent between devices in bfloat16 or wider.
A program may use at most 1 GiB of HBM per device.

```python
import jax
import jax.numpy as jnp
from jax import lax

BATCH_SIZE = 12
IMG_TOKENS = 1024
TEXT_TOKENS = 128
D_MODEL = 2048
NUM_HEADS = 8
HEAD_DIM = 256
FF_DIM = 16384

SEQ_LEN = IMG_TOKENS + TEXT_TOKENS
QUERY_WIDTH = NUM_HEADS * HEAD_DIM
QUERY_SCALE = HEAD_DIM ** -0.5
NORM_EPS = 1e-6
ROPE_BASE = 10000.0
MASK_FILL = -1e30


def setup_inputs(seed: int = 0, part: int = 0) -> dict:
    base_key = jax.random.key(seed)
    part_keys = jax.random.split(jax.random.fold_in(base_key, part), 4)
    weight_keys = jax.random.split(base_key, 10)
    noise_rows = jax.random.normal(part_keys[0], (BATCH_SIZE, SEQ_LEN, D_MODEL), jnp.float32)
    text_dir = jax.random.normal(part_keys[1], (BATCH_SIZE, 1, D_MODEL), jnp.float32)
    is_text = (jnp.arange(SEQ_LEN) >= IMG_TOKENS).astype(jnp.float32)[None, :, None]
    hidden = noise_rows + 2.0 * text_dir * is_text
    prompt_len = jax.random.randint(part_keys[2], (BATCH_SIZE,), 1, TEXT_TOKENS // 2 + 1)
    prefix_len = IMG_TOKENS + prompt_len
    valid_len = prefix_len + jax.random.randint(part_keys[3], (BATCH_SIZE,), 1, SEQ_LEN - prefix_len + 1)
    attn_gain = SEQ_LEN ** 0.5 / 6.0

    def draw_weight(key_index, shape, scale):
        return (jax.random.normal(weight_keys[key_index], shape, jnp.float32) * scale).astype(jnp.bfloat16)

    return {
        "hidden": hidden.astype(jnp.bfloat16),
        "prefix_len": prefix_len.astype(jnp.int32),
        "valid_len": valid_len.astype(jnp.int32),
        "norm_attn": draw_weight(0, (D_MODEL,), 0.3),
        "w_query": draw_weight(1, (D_MODEL, QUERY_WIDTH), 1.5 * D_MODEL ** -0.5),
        "w_key": draw_weight(2, (D_MODEL, HEAD_DIM), D_MODEL ** -0.5),
        "w_value": draw_weight(3, (D_MODEL, HEAD_DIM), D_MODEL ** -0.5),
        "w_out": draw_weight(4, (QUERY_WIDTH, D_MODEL), attn_gain * QUERY_WIDTH ** -0.5),
        "norm_mlp": draw_weight(5, (D_MODEL,), 0.3),
        "w_gate": draw_weight(6, (D_MODEL, FF_DIM), D_MODEL ** -0.5),
        "w_up": draw_weight(7, (D_MODEL, FF_DIM), D_MODEL ** -0.5),
        "w_down": draw_weight(8, (FF_DIM, D_MODEL), FF_DIM ** -0.5),
    }


def rms_norm(acts, norm_scale):
    acts_f32 = acts.astype(jnp.float32)
    inv_rms = lax.rsqrt(jnp.mean(acts_f32 * acts_f32, axis=-1, keepdims=True) + NORM_EPS)
    return (acts_f32 * inv_rms * (1.0 + norm_scale.astype(jnp.float32))).astype(jnp.bfloat16)


def rope_tables(positions):
    half_dim = HEAD_DIM // 2
    inv_freq = ROPE_BASE ** (-2.0 * jnp.arange(half_dim, dtype=jnp.float32) / HEAD_DIM)
    angles = positions.astype(jnp.float32)[:, None] * inv_freq[None, :]
    return jnp.cos(angles), jnp.sin(angles)


def apply_rope(vectors, cos_table, sin_table):
    half_dim = vectors.shape[-1] // 2
    first_half = vectors[..., :half_dim]
    second_half = vectors[..., half_dim:]
    return jnp.concatenate([first_half * cos_table - second_half * sin_table, second_half * cos_table + first_half * sin_table], axis=-1)


def reference(hidden, prefix_len, valid_len, norm_attn, w_query, w_key, w_value, w_out, norm_mlp, w_gate, w_up, w_down):
    positions = jnp.arange(SEQ_LEN)
    cos_table, sin_table = rope_tables(positions)
    row_pos = positions[:, None]
    col_pos = positions[None, :]

    def one_sample(sample_args):
        sample_rows, sample_prefix, sample_valid = sample_args
        normed = rms_norm(sample_rows, norm_attn)
        query_rows = jnp.dot(normed, w_query, preferred_element_type=jnp.float32).reshape(SEQ_LEN, NUM_HEADS, HEAD_DIM)
        query_rows = (apply_rope(query_rows, cos_table[:, None, :], sin_table[:, None, :]) * QUERY_SCALE).astype(jnp.bfloat16)
        key_rows = apply_rope(jnp.dot(normed, w_key, preferred_element_type=jnp.float32), cos_table, sin_table).astype(jnp.bfloat16)
        value_rows = jnp.dot(normed, w_value, preferred_element_type=jnp.float32).astype(jnp.bfloat16)
        allowed = (col_pos < sample_valid) & ((col_pos < sample_prefix) | (col_pos <= row_pos))

        def one_head(query_head):
            scores = jnp.dot(query_head, key_rows.T, preferred_element_type=jnp.float32)
            scores = jnp.where(allowed, scores, MASK_FILL)
            attn_probs = jax.nn.softmax(scores, axis=-1).astype(jnp.bfloat16)
            return jnp.dot(attn_probs, value_rows, preferred_element_type=jnp.float32).astype(jnp.bfloat16)

        attn_vals = lax.map(one_head, jnp.transpose(query_rows, (1, 0, 2)))
        attn_flat = jnp.transpose(attn_vals, (1, 0, 2)).reshape(SEQ_LEN, QUERY_WIDTH)
        attn_out = jnp.dot(attn_flat, w_out, preferred_element_type=jnp.float32).astype(jnp.bfloat16)
        hidden_mid = (sample_rows.astype(jnp.float32) + attn_out.astype(jnp.float32)).astype(jnp.bfloat16)
        normed_mlp = rms_norm(hidden_mid, norm_mlp)
        gate_proj = jnp.dot(normed_mlp, w_gate, preferred_element_type=jnp.float32)
        up_proj = jnp.dot(normed_mlp, w_up, preferred_element_type=jnp.float32)
        mlp_act = (jax.nn.gelu(gate_proj, approximate=True) * up_proj).astype(jnp.bfloat16)
        mlp_out = jnp.dot(mlp_act, w_down, preferred_element_type=jnp.float32).astype(jnp.bfloat16)
        hidden_out = (hidden_mid.astype(jnp.float32) + mlp_out.astype(jnp.float32)).astype(jnp.bfloat16)
        return hidden_out, key_rows, value_rows

    hidden_out, key_cache, value_cache = lax.map(one_sample, (hidden, prefix_len, valid_len))
    return (hidden_out, key_cache, value_cache)
```

```python
import functools

import jax
import jax.numpy as jnp
import numpy as np
from jax import lax
from jax.experimental import pallas as pl
from jax.experimental.pallas import tpu as pltpu
from jax.sharding import PartitionSpec as P

NORM_EPS = 1e-6
ROPE_BASE = 10000.0
MASK_FILL = -1e30
F32 = jnp.float32
BF16 = jnp.bfloat16
MESH = pl.DeviceIdType.MESH
VMEM_LIMIT = 67043328


def rope_tables(seq, head_dim):
    inv_freq = ROPE_BASE ** (-2.0 * np.arange(head_dim // 2) / head_dim)
    angles = np.arange(seq)[:, None] * inv_freq[None, :]
    return np.cos(angles).astype(np.float32), np.sin(angles).astype(np.float32)


def normalize(rows, gain):
    inv = lax.rsqrt(jnp.mean(rows * rows, axis=-1, keepdims=True) + NORM_EPS)
    return (rows * inv * (1.0 + gain)).astype(BF16)


def dot(a, b):
    return jnp.dot(a, b, preferred_element_type=F32)


def span(index, size):
    return pl.ds(pl.multiple_of(index * size, size), size)


def start(copies):
    for c in copies:
        c.start()


def wait_recv(copies):
    for c in copies:
        c.wait_recv()


def wait_send(copies):
    for c in copies:
        c.wait_send()


def send(src, dst, send_sem, recv_sem, peer):
    return pltpu.make_async_remote_copy(src_ref=src, dst_ref=dst, send_sem=send_sem, recv_sem=recv_sem, device_id=peer, device_id_type=MESH)


def peers():
    dp = lax.axis_index("dp")
    tp = lax.axis_index("tp")
    core_tp = tp + 1 - 2 * lax.rem(tp, 2)
    chip_tp = lax.rem(tp + 2, 4)
    return dp, tp, chip_tp, {"tp": core_tp}, {"tp": chip_tp}, {"dp": 1 - dp}


def enter(*others):
    barrier = pltpu.get_barrier_semaphore()
    for peer in others:
        pl.semaphore_signal(barrier, inc=1, device_id=peer, device_id_type=MESH)
    pl.semaphore_wait(barrier, len(others))


Q_PIECES = 2
O_PIECES = 4


def attention_kernel(plen_ref, vlen_ref, gain_ref, h_hbm, cos_hbm, sin_hbm, wq_hbm, wk_hbm, wv_hbm, wo_hbm,
                     h1_hbm, key_hbm, value_hbm, wo_far,
                     x_v, q_v, kv_v, w_v, wkv_v, cos_v, sin_v,
                     table_sem, x_sem, wkv_sem, w_sem, out_sem, key_sem,
                     qc_send, qc_recv, qx_send, qx_recv, qy_send, qy_recv, qxc_send, qxc_recv, qyc_send, qyc_recv,
                     oc_send, oc_recv, ox_send, ox_recv, oy_send, oy_recv, oxc_send, oxc_recv, oyc_send, oyc_recv,
                     kx_send, kx_recv, kc_send, kc_recv, kxc_send, kxc_recv):
    num_batch, rows, width = x_v.shape
    heads, hd = q_v.shape[1], q_v.shape[3]
    seq = kv_v.shape[1]
    own_heads = wq_hbm.shape[1] // hd
    half = hd // 2
    dp, tp, chip_tp, core_peer, chip_peer, group_peer = peers()
    own_rows = span(tp, rows)
    chip_rows = span(chip_tp, rows)

    tables = [pltpu.make_async_copy(t.at[own_rows], v, table_sem.at[i]) for i, (t, v) in enumerate(((cos_hbm, cos_v), (sin_hbm, sin_v)))]
    wkv = [pltpu.make_async_copy(w, wkv_v.at[i], wkv_sem.at[i]) for i, w in enumerate((wk_hbm, wv_hbm))]
    own_q = [pltpu.make_async_copy(wq_hbm.at[:, pl.ds(i * hd, hd)], w_v.at[i], w_sem.at[i, 0]) for i in range(own_heads)]

    def x_load(s):
        return pltpu.make_async_copy(h_hbm.at[s], x_v.at[s], x_sem.at[s])

    def own_o(n):
        return pltpu.make_async_copy(wo_hbm.at[:, pl.ds(n * hd, hd)], w_v.at[n, pl.ds(0, own_heads * hd)], w_sem.at[n, 0])

    def far_o(n):
        size = (heads - own_heads) * hd
        return pltpu.make_async_copy(wo_far.at[:, pl.ds(n * hd, hd)], w_v.at[n, pl.ds(own_heads * hd, size)], w_sem.at[n, 1])

    q_core = [send(wq_hbm.at[:, pl.ds(i * hd, hd)], w_v.at[own_heads + i], qc_send.at[i], qc_recv.at[i], core_peer) for i in range(own_heads)]
    q_rows = width // Q_PIECES

    def q_chip(i):
        return send(wq_hbm.at[pl.ds(i * q_rows, q_rows), span(dp, hd)], w_v.at[4, pl.ds(i * q_rows, q_rows)], qx_send.at[i], qx_recv.at[i], chip_peer)

    def q_move(src, dst, i, send_sem, recv_sem, peer):
        at = pl.ds(i * q_rows, q_rows)
        return send(w_v.at[src, at], w_v.at[dst, at], send_sem.at[i], recv_sem.at[i], peer)

    def q_group(i):
        return q_move(4, 6, i, qy_send, qy_recv, group_peer)

    def q_chip_core(i):
        return q_move(4, 5, i, qxc_send, qxc_recv, core_peer)

    def q_group_core(i):
        return q_move(6, 7, i, qyc_send, qyc_recv, core_peer)

    own_width = own_heads * hd
    o_rows = hd // O_PIECES
    o_core = [send(wo_hbm, wo_far.at[pl.ds(0, own_width)], oc_send.at[0], oc_recv.at[0], core_peer)]

    def far_rows(slot, i):
        return wo_far.at[pl.ds((slot - own_heads) * hd + i * o_rows, o_rows)]

    def o_chip(i):
        src = wo_hbm.at[pl.ds(pl.multiple_of(dp * hd + i * o_rows, o_rows), o_rows)]
        return send(src, far_rows(4, i), ox_send.at[i], ox_recv.at[i], chip_peer)

    def o_group(i):
        return send(far_rows(4, i), far_rows(6, i), oy_send.at[i], oy_recv.at[i], group_peer)

    def o_chip_core(i):
        return send(far_rows(4, i), far_rows(5, i), oxc_send.at[i], oxc_recv.at[i], core_peer)

    def o_group_core(i):
        return send(far_rows(6, i), far_rows(7, i), oyc_send.at[i], oyc_recv.at[i], core_peer)

    def kv_chip(s):
        return send(kv_v.at[s, own_rows], kv_v.at[s, own_rows], kx_send.at[s], kx_recv.at[s], chip_peer)

    def kv_core(s):
        return send(kv_v.at[s, own_rows], kv_v.at[s, own_rows], kc_send.at[s], kc_recv.at[s], core_peer)

    def kv_chip_core(s):
        return send(kv_v.at[s, chip_rows], kv_v.at[s, chip_rows], kxc_send.at[s], kxc_recv.at[s], core_peer)

    def kv_stores(s):
        outs = ((key_hbm, 0), (value_hbm, hd))
        return [pltpu.make_async_copy(kv_v.at[s, own_rows, pl.ds(at, hd)], ref.at[s], key_sem.at[s, i]) for i, (ref, at) in enumerate(outs)]

    def kv_send(s):
        kv_chip(s).start()
        kv_core(s).start()
        start(kv_stores(s))

    x_load(0).start()
    start(wkv + tables + own_q)

    @pl.loop(1, num_batch)
    def _(s):
        x_load(s).start()

    enter(core_peer, chip_peer, group_peer)
    start([q_chip(i) for i in range(Q_PIECES)])
    start(q_core)
    start([o_chip(i) for i in range(O_PIECES)])
    start(o_core)

    for c in tables + wkv + own_q:
        c.wait()
    gain = gain_ref[...].astype(F32)

    def rope(x, cos, sin):
        a, c = x[:, :half], x[:, half:]
        return a * cos - c * sin, c * cos + a * sin

    def store_query(q, cos, sin, at, slot):
        lo, hi = rope(q, cos, sin)
        shape = q_v[at, slot, :, :half].shape
        q_v[at, slot, :, :half] = lo.astype(BF16).reshape(shape)
        q_v[at, slot, :, half:] = hi.astype(BF16).reshape(shape)

    @pl.loop(0, num_batch)
    def _(s):
        @pl.when(s == 5)
        def _():
            q_chip(0).wait_recv()
            start([q_group(0), q_chip_core(0)])

        @pl.when(s == num_batch - 1)
        def _():
            for i in range(1, Q_PIECES):
                q_chip(i).wait_recv()
                start([q_group(i), q_chip_core(i)])

        @pl.when(s > 0)
        def _():
            kv_send(s - 1)

        x_load(s).wait()
        xn = normalize(x_v[s].astype(F32), gain)
        x_v[s] = xn
        cos, sin = cos_v[...], sin_v[...]
        lo, hi = rope(dot(xn, wkv_v[0]), cos, sin)
        kv_v[s, own_rows, :half] = lo.astype(BF16)
        kv_v[s, own_rows, half:hd] = hi.astype(BF16)
        kv_v[s, own_rows, hd:] = dot(xn, wkv_v[1]).astype(BF16)
        for i in range(own_heads):
            store_query(dot(xn, w_v[i]), cos * hd**-0.5, sin * hd**-0.5, s, i)

    kv_send(num_batch - 1)

    group = 3

    @pl.loop(own_heads, heads)
    def _(slot):
        @pl.when(slot == 2)
        def _():
            wait_recv(q_core)

        @pl.when(slot == 3)
        def _():
            o_chip(0).wait_recv()
            start([o_group(0), o_chip_core(0)])

        @pl.when(slot == 5)
        def _():
            wait_recv([q_chip_core(i) for i in range(Q_PIECES)])
            o_chip(1).wait_recv()
            start([o_group(1), o_chip_core(1)])

        @pl.when(slot == 6)
        def _():
            for i in range(Q_PIECES):
                q_group(i).wait_recv()
                q_group_core(i).start()
            o_chip(2).wait_recv()
            start([o_group(2), o_chip_core(2)])

        @pl.when(slot == 7)
        def _():
            wait_recv([q_group_core(i) for i in range(Q_PIECES)])
            o_chip(3).wait_recv()
            start([o_group(3), o_chip_core(3)])

        @pl.loop(0, num_batch // group)
        def _(i):
            at = span(i, group)
            cos = jnp.concatenate([cos_v[...] * hd**-0.5] * group, axis=0)
            sin = jnp.concatenate([sin_v[...] * hd**-0.5] * group, axis=0)
            store_query(dot(x_v[at].reshape(group * rows, width), w_v[slot]), cos, sin, at, slot)

    for copies in ([q_group(i) for i in range(Q_PIECES)], [q_chip_core(i) for i in range(Q_PIECES)], [q_group_core(i) for i in range(Q_PIECES)]):
        wait_send(copies)
    for n in range(heads):
        own_o(n).start()

    @pl.loop(0, num_batch)
    def _(s):
        x_load(s).start()

    kv_chip(0).wait_recv()
    kv_chip_core(0).start()
    for i in range(O_PIECES):
        o_group(i).wait_recv()
        o_group_core(i).start()
    wait_recv(o_core + [o_chip_core(i) for i in range(O_PIECES)] + [o_group_core(i) for i in range(O_PIECES)])
    for n in range(heads):
        far_o(n).start()

    tail = 128
    col = lax.broadcasted_iota(jnp.int32, (rows, tail), 1) + (seq - tail)
    row = lax.broadcasted_iota(jnp.int32, (rows, tail), 0) + tp * rows

    def score(s, p):
        return lax.dot_general(q_v[s, p], kv_v[s, :, :hd], (((1,), (1,)), ((), ())), preferred_element_type=F32)

    def probs(sc, allowed):
        sc = jnp.concatenate([sc[:, : seq - tail], jnp.where(allowed, sc[:, seq - tail :], MASK_FILL)], axis=1)
        p = jnp.exp(sc - jnp.max(sc, axis=-1, keepdims=True))
        return (p * (1.0 / jnp.sum(p, axis=-1, keepdims=True))).astype(BF16)

    def project(s, n):
        o = jnp.concatenate([q_v[s, j] for j in range(heads)], axis=1)
        at = slice(n * hd, (n + 1) * hd)
        x_v[s, :, at] = (x_v[s, :, at].astype(F32) + dot(o, w_v[n]).astype(BF16).astype(F32)).astype(BF16)

    def out_store(s):
        return pltpu.make_async_copy(x_v.at[s], h1_hbm.at[s], out_sem.at[s])

    def attend(s, project_too):
        wait_recv([kv_core(s), kv_chip_core(s)])
        allowed = (col < vlen_ref[s]) & ((col < plen_ref[s]) | (col <= row))
        if project_too:
            x_load(s - 1).wait()
        for first in (0, heads // 2):
            if first:

                @pl.when(s < num_batch - 1)
                def _():
                    kv_chip(s + 1).wait_recv()
                    kv_chip_core(s + 1).start()

            sc = score(s, first)
            for p in range(first, first + heads // 2):
                ahead = score(s, p + 1) if p + 1 < first + heads // 2 else None
                if project_too:
                    project(s - 1, p)
                q_v[s, p] = dot(probs(sc, allowed), kv_v[s, :, hd:]).astype(BF16)
                sc = ahead
        if project_too:
            out_store(s - 1).start()

    attend(0, False)
    for n in range(heads):
        own_o(n).wait()
        far_o(n).wait()

    @pl.loop(1, num_batch)
    def _(s):
        attend(s, True)

    x_load(num_batch - 1).wait()
    for n in range(heads):
        project(num_batch - 1, n)
    out_store(num_batch - 1).start()

    wait_send(q_core + o_core + [q_chip(i) for i in range(Q_PIECES)])
    for i in range(O_PIECES):
        wait_send([o_chip(i), o_group(i), o_chip_core(i), o_group_core(i)])

    @pl.loop(0, num_batch)
    def _(s):
        wait_send([kv_chip(s), kv_core(s), kv_chip_core(s)])
        for c in kv_stores(s):
            c.wait()
        out_store(s).wait()


def attention(hidden, prefix_len, valid_len, norm_attn, w_query, w_key, w_value, w_out, tp_size):
    num_batch, rows, width = hidden.shape
    hd = w_key.shape[1]
    own_heads = w_query.shape[1] // hd
    heads = own_heads * tp_size
    seq = rows * tp_size
    cos, sin = rope_tables(seq, hd)
    any_spec = pl.BlockSpec(memory_space=pl.ANY)
    smem = pl.BlockSpec(memory_space=pltpu.SMEM)
    dma = pltpu.SemaphoreType.DMA
    shape = jax.ShapeDtypeStruct
    flops = 2 * num_batch * rows * (width * (2 * heads + 2) * hd + 2 * heads * hd * seq)
    out = pl.pallas_call(
        attention_kernel,
        in_specs=[smem, smem, pl.BlockSpec(memory_space=pltpu.VMEM)] + [any_spec] * 7,
        out_specs=[any_spec] * 4,
        out_shape=[
            shape((num_batch, rows, width), BF16),
            shape((num_batch, rows, hd), BF16),
            shape((num_batch, rows, hd), BF16),
            shape(((heads - own_heads) * hd, width), BF16),
        ],
        scratch_shapes=[
            pltpu.VMEM((num_batch, rows, width), BF16),
            pltpu.VMEM((num_batch, heads, rows, hd), BF16),
            pltpu.VMEM((num_batch, seq, 2 * hd), BF16),
            pltpu.VMEM((heads, width, hd), BF16),
            pltpu.VMEM((2, width, hd), BF16),
            pltpu.VMEM((rows, hd // 2), F32),
            pltpu.VMEM((rows, hd // 2), F32),
            dma((2,)),
            dma((num_batch,)),
            dma((2,)),
            dma((heads, 2)),
            dma((num_batch,)),
            dma((num_batch, 2)),
        ]
        + [dma((own_heads,))] * 2
        + [dma((Q_PIECES,))] * 8
        + [dma((1,))] * 2
        + [dma((O_PIECES,))] * 8
        + [dma((num_batch,))] * 6,
        compiler_params=pltpu.CompilerParams(vmem_limit_bytes=VMEM_LIMIT, collective_id=1, has_side_effects=True),
        cost_estimate=pl.CostEstimate(flops=flops, bytes_accessed=num_batch * rows * width * 6, transcendentals=num_batch * rows * heads * seq),
        name="attention",
    )(prefix_len, valid_len, norm_attn.reshape(1, width), hidden, jnp.asarray(cos), jnp.asarray(sin), w_query, w_key, w_value, w_out)
    return out[:3]


def mlp_kernel(gain_ref, h_hbm, wg_hbm, wu_hbm, wd_hbm, out_hbm, pg_hbm, pu_hbm, pd_hbm, rg_hbm, ru_hbm, rd_hbm,
               x_v, acc_v, act_v, wg_v, wu_v, wd_v, load_sem, x_sem, out_sem,
               p_send, p_recv, a_send, a_recv, ac_send, ac_recv, b_send, b_recv, bc_send, bc_recv):
    rows, width = x_v.shape
    tile = act_v.shape[0]
    tiles = rows // tile
    unit = wg_v.shape[2]
    piece = unit // 2
    own = wg_hbm.shape[1] // unit
    pieces = own // 2 * 2
    groups, per_group = rg_hbm.shape[:2]
    steps = 2 * own + groups * per_group
    dp, tp, chip_tp, core_peer, chip_peer, group_peer = peers()

    def piece_refs(group, j):
        at = pl.ds(pl.multiple_of(lax.rem(j, 2) * piece, piece), piece)
        return rg_hbm.at[group, j // 2, :, at], ru_hbm.at[group, j // 2, :, at], rd_hbm.at[group, j // 2, at, :]

    def own_copies():
        refs = ((wg_hbm, pg_hbm), (wu_hbm, pu_hbm), (wd_hbm, pd_hbm))
        return [send(src, dst, p_send.at[i], p_recv.at[i], core_peer) for i, (src, dst) in enumerate(refs)]

    def chip_copies(j):
        at = pl.ds(pl.multiple_of(dp * pieces * piece + j * piece, piece), piece)
        src = (wg_hbm.at[:, at], wu_hbm.at[:, at], wd_hbm.at[at, :])
        return [send(s, d, a_send.at[j, i], a_recv.at[j, i], chip_peer) for i, (s, d) in enumerate(zip(src, piece_refs(0, j)))]

    def relay(j, source, target, send_sems, recv_sems, peer):
        pairs = zip(piece_refs(source, j), piece_refs(target, j))
        return [send(s, d, send_sems.at[j, i], recv_sems.at[j, i], peer) for i, (s, d) in enumerate(pairs)]

    def core_a(j):
        return relay(j, 0, 1, ac_send, ac_recv, core_peer)

    def group_a(j):
        return relay(j, 0, 2, b_send, b_recv, group_peer)

    def core_b(j):
        return relay(j, 2, 3, bc_send, bc_recv, core_peer)

    def h_copy(m):
        at = span(m, tile)
        return pltpu.make_async_copy(h_hbm.at[at], x_v.at[at], x_sem.at[m])

    def load(src, slot):
        return [pltpu.make_async_copy(s, d.at[slot], load_sem.at[slot, i]) for i, (s, d) in enumerate(zip(src, (wg_v, wu_v, wd_v)))]

    def own_load(u, slot):
        at = pl.ds(pl.multiple_of(u * unit, unit), unit)
        return load((wg_hbm.at[:, at], wu_hbm.at[:, at], wd_hbm.at[at, :]), slot)

    def peer_load(u, slot):
        at = pl.ds(pl.multiple_of((u - own) * unit, unit), unit)
        return load((pg_hbm.at[:, at], pu_hbm.at[:, at], pd_hbm.at[at, :]), slot)

    def far_load(u, slot):
        i = u - 2 * own
        g = lax.rem(i, groups)
        p = i // groups
        return load((rg_hbm.at[g, p], ru_hbm.at[g, p], rd_hbm.at[g, p]), slot)

    for m in range(tiles):
        h_copy(m).start()
    start(own_load(0, 0))
    enter(core_peer, chip_peer, group_peer)
    start(own_copies())

    @pl.loop(0, pieces)
    def _(j):
        start(chip_copies(j))

    acc_v[...] = jnp.zeros_like(acc_v)
    gain = gain_ref[...].astype(F32)
    for m in range(tiles):
        h_copy(m).wait()

        @pl.loop(0, tile // 96)
        def _(i):
            at = span(m * (tile // 96) + i, 96)
            x_v[at, :] = normalize(x_v[at, :].astype(F32), gain)

    def out_copy(m):
        at = pl.ds(pl.multiple_of(m * tile, tile), tile)
        return pltpu.make_async_copy(x_v.at[at], out_hbm.at[at], out_sem.at[m])

    def finish(m):
        h_copy(m).wait()
        chunk = 48

        @pl.loop(0, tile // chunk)
        def _(i):
            at = pl.ds(pl.multiple_of(m * tile + i * chunk, chunk), chunk)
            x_v[at, :] = (x_v[at, :].astype(F32) + acc_v[at, :].astype(BF16).astype(F32)).astype(BF16)

        out_copy(m).start()

    first_a, first_b, every = 4, 8, 3

    @pl.loop(0, steps)
    def _(s):
        slot = lax.rem(s, 2)

        @pl.when((s >= first_a) & (s < first_a + every * pieces) & (lax.rem(s - first_a + every, every) == 0))
        def _():
            j = (s - first_a) // every
            wait_recv(chip_copies(j))
            start(group_a(j))
            start(core_a(j))

        @pl.when((s >= first_b) & (s < first_b + every * pieces) & (lax.rem(s - first_b + 2 * every, every) == 0))
        def _():
            j = (s - first_b) // every
            wait_recv(group_a(j))
            start(core_b(j))

        u = s + 1

        @pl.when(u < own)
        def _():
            start(own_load(u, 1 - slot))

        @pl.when(u == own)
        def _():
            wait_recv(own_copies())

        @pl.when((u >= own) & (u < 2 * own))
        def _():
            start(peer_load(u, 1 - slot))

        @pl.when((u >= 2 * own) & (u < steps))
        def _():
            g = lax.rem(u - 2 * own, groups)
            p = (u - 2 * own) // groups

            @pl.when(g == 1)
            def _():
                for j in (2 * p, 2 * p + 1):
                    wait_recv(core_a(j))

            @pl.when(g == 3)
            def _():
                for j in (2 * p, 2 * p + 1):
                    wait_recv(core_b(j))

            start(far_load(u, 1 - slot))

        for c in own_load(0, slot):
            c.wait()

        @pl.loop(0, tiles)
        def _(m):
            at = pl.ds(pl.multiple_of(m * tile, tile), tile)
            gate = dot(x_v[at, :], wg_v[slot])
            up = dot(x_v[at, :], wu_v[slot])
            act_v[...] = (jax.nn.gelu(gate, approximate=True) * up).astype(BF16)
            for n in range(0, width, unit):
                acc_v[at, n : n + unit] += dot(act_v[...], wd_v[slot, :, n : n + unit])

            @pl.when(s == steps - 1)
            def _():
                h_copy(m).start()

                @pl.when(m > 0)
                def _():
                    finish(m - 1)

    finish(tiles - 1)
    wait_send(own_copies())

    @pl.loop(0, pieces)
    def _(j):
        for copies in (chip_copies(j), group_a(j), core_a(j), core_b(j)):
            wait_send(copies)

    for m in range(tiles):
        out_copy(m).wait()


def mlp(h1, norm_mlp, w_gate, w_up, w_down):
    rows, width = h1.shape
    ff = w_gate.shape[1]
    unit = 512
    tile = rows // 3
    far = ff // 2 // unit
    pieces = 2 * far
    shapes = [(rows, width), (width, ff), (width, ff), (ff, width), (4, far, width, unit), (4, far, width, unit), (4, far, unit, width)]
    any_spec = pl.BlockSpec(memory_space=pl.ANY)
    dma = pltpu.SemaphoreType.DMA
    out = pl.pallas_call(
        mlp_kernel,
        in_specs=[pl.BlockSpec(memory_space=pltpu.VMEM)] + [any_spec] * 4,
        out_specs=[any_spec] * 7,
        out_shape=[jax.ShapeDtypeStruct(s, BF16) for s in shapes],
        scratch_shapes=[
            pltpu.VMEM((rows, width), BF16),
            pltpu.VMEM((rows, width), F32),
            pltpu.VMEM((tile, unit), BF16),
            pltpu.VMEM((2, width, unit), BF16),
            pltpu.VMEM((2, width, unit), BF16),
            pltpu.VMEM((2, unit, width), BF16),
            dma((2, 3)),
            dma((rows // tile,)),
            dma((rows // tile,)),
            dma((3,)),
            dma((3,)),
        ]
        + [dma((pieces, 3))] * 8,
        compiler_params=pltpu.CompilerParams(vmem_limit_bytes=VMEM_LIMIT, collective_id=0, has_side_effects=True),
        cost_estimate=pl.CostEstimate(flops=2 * rows * width * ff * 3 * 4, bytes_accessed=4 * 3 * width * ff * 2, transcendentals=0),
        name="mlp",
    )(norm_mlp.reshape(1, width), h1, w_gate, w_up, w_down)
    return out[0]


def solution(mesh):
    tp_size = mesh.shape["tp"]
    row_spec = P("dp", "tp", None)
    arg_specs = (row_spec, P("dp"), P("dp"), P(), P(None, "tp"), P(), P(), P("tp", None), P(), P(None, "tp"), P(None, "tp"), P("tp", None))

    def local_layer(hidden, prefix_len, valid_len, norm_attn, w_query, w_key, w_value, w_out, norm_mlp, w_gate, w_up, w_down):
        h1, key, value = attention(hidden, prefix_len, valid_len, norm_attn, w_query, w_key, w_value, w_out, tp_size)
        out = mlp(h1.reshape(-1, hidden.shape[-1]), norm_mlp, w_gate, w_up, w_down)
        return out.reshape(hidden.shape), key, value

    return jax.shard_map(local_layer, mesh=mesh, in_specs=arg_specs, out_specs=(row_spec, row_spec, row_spec), check_vma=False)
```

```python
import functools

import jax
import jax.numpy as jnp
import numpy as np
from jax import lax
from jax.experimental import pallas as pl
from jax.experimental.pallas import tpu as pltpu
from jax.sharding import PartitionSpec as P

NORM_EPS = 1e-6
ROPE_BASE = 10000.0
MASK_FILL = -1e30
F32 = jnp.float32
BF16 = jnp.bfloat16
MESH = pl.DeviceIdType.MESH
VMEM_LIMIT = 67043328


def rope_tables(rows, blocks, head_dim):
    inv_freq = ROPE_BASE ** (-2.0 * np.arange(head_dim // 2) / head_dim)
    angles = np.arange(rows)[:, None] * inv_freq[None, :]
    starts = np.arange(blocks)[:, None] * rows * inv_freq[None, :]
    return tuple(f(a).astype(np.float32) for a in (angles, starts) for f in (np.cos, np.sin))


def normalize(rows, gain):
    inv = lax.rsqrt(jnp.mean(rows * rows, axis=-1, keepdims=True) + NORM_EPS)
    return (rows * inv * (1.0 + gain)).astype(BF16)


def dot(a, b):
    return jnp.dot(a, b, preferred_element_type=F32)


def span(index, size):
    return pl.ds(pl.multiple_of(index * size, size), size)


def start(copies):
    for c in copies:
        c.start()


def wait_recv(copies):
    for c in copies:
        c.wait_recv()


def wait_send(copies):
    for c in copies:
        c.wait_send()


def send(src, dst, send_sem, recv_sem, peer):
    return pltpu.make_async_remote_copy(src_ref=src, dst_ref=dst, send_sem=send_sem, recv_sem=recv_sem, device_id=peer, device_id_type=MESH)


def peers():
    dp = lax.axis_index("dp")
    tp = lax.axis_index("tp")
    core_tp = tp + 1 - 2 * lax.rem(tp, 2)
    chip_tp = lax.rem(tp + 2, 4)
    return dp, tp, chip_tp, {"tp": core_tp}, {"tp": chip_tp}, {"dp": 1 - dp}


def enter(*others):
    barrier = pltpu.get_barrier_semaphore()
    for peer in others:
        pl.semaphore_signal(barrier, inc=1, device_id=peer, device_id_type=MESH)
    pl.semaphore_wait(barrier, len(others))


Q_PIECES = 2
O_PIECES = 4


def attention_kernel(plen_ref, vlen_ref, gain_ref, gain2_ref, h_hbm, cos_ref, sin_ref, cos0_ref, sin0_ref, wq_hbm, wk_hbm, wv_hbm, wo_hbm,
                     h1_hbm, x2_hbm, key_hbm, value_hbm, wo_far,
                     x_v, q_v, kv_v, w_v, wkv_v, cos_v, sin_v, x2_v,
                     x_sem, wkv_sem, w_sem, out_sem, x2_sem, key_sem,
                     qc_send, qc_recv, qx_send, qx_recv, qy_send, qy_recv, qxc_send, qxc_recv, qyc_send, qyc_recv,
                     oc_send, oc_recv, ox_send, ox_recv, oy_send, oy_recv, oxc_send, oxc_recv, oyc_send, oyc_recv,
                     kx_send, kx_recv, kc_send, kc_recv, kxc_send, kxc_recv):
    num_batch, rows, width = x_v.shape
    heads, hd = q_v.shape[1], q_v.shape[3]
    seq = kv_v.shape[1]
    own_heads = wq_hbm.shape[1] // hd
    half = hd // 2
    dp, tp, chip_tp, core_peer, chip_peer, group_peer = peers()
    own_rows = span(tp, rows)
    chip_rows = span(chip_tp, rows)

    wkv = [pltpu.make_async_copy(w, wkv_v.at[i], wkv_sem.at[i]) for i, w in enumerate((wk_hbm, wv_hbm))]
    own_q = [pltpu.make_async_copy(wq_hbm.at[:, pl.ds(i * hd, hd)], w_v.at[i], w_sem.at[i, 0]) for i in range(own_heads)]

    def x_load(s):
        return pltpu.make_async_copy(h_hbm.at[s], x_v.at[s], x_sem.at[s])

    def own_o(n):
        return pltpu.make_async_copy(wo_hbm.at[:, pl.ds(n * hd, hd)], w_v.at[n, pl.ds(0, own_heads * hd)], w_sem.at[n, 0])

    def far_o(n):
        size = (heads - own_heads) * hd
        return pltpu.make_async_copy(wo_far.at[:, pl.ds(n * hd, hd)], w_v.at[n, pl.ds(own_heads * hd, size)], w_sem.at[n, 1])

    q_core = [send(wq_hbm.at[:, pl.ds(i * hd, hd)], w_v.at[own_heads + i], qc_send.at[i], qc_recv.at[i], core_peer) for i in range(own_heads)]
    q_rows = width // Q_PIECES

    def q_chip(i):
        return send(wq_hbm.at[pl.ds(i * q_rows, q_rows), span(dp, hd)], w_v.at[4, pl.ds(i * q_rows, q_rows)], qx_send.at[i], qx_recv.at[i], chip_peer)

    def q_move(src, dst, i, send_sem, recv_sem, peer):
        at = pl.ds(i * q_rows, q_rows)
        return send(w_v.at[src, at], w_v.at[dst, at], send_sem.at[i], recv_sem.at[i], peer)

    def q_group(i):
        return q_move(4, 6, i, qy_send, qy_recv, group_peer)

    def q_chip_core(i):
        return q_move(4, 5, i, qxc_send, qxc_recv, core_peer)

    def q_group_core(i):
        return q_move(6, 7, i, qyc_send, qyc_recv, core_peer)

    own_width = own_heads * hd
    o_rows = hd // O_PIECES
    o_core = [send(wo_hbm, wo_far.at[pl.ds(0, own_width)], oc_send.at[0], oc_recv.at[0], core_peer)]

    def far_rows(slot, i):
        return wo_far.at[pl.ds((slot - own_heads) * hd + i * o_rows, o_rows)]

    def o_chip(i):
        src = wo_hbm.at[pl.ds(pl.multiple_of(dp * hd + i * o_rows, o_rows), o_rows)]
        return send(src, far_rows(4, i), ox_send.at[i], ox_recv.at[i], chip_peer)

    def o_group(i):
        return send(far_rows(4, i), far_rows(6, i), oy_send.at[i], oy_recv.at[i], group_peer)

    def o_chip_core(i):
        return send(far_rows(4, i), far_rows(5, i), oxc_send.at[i], oxc_recv.at[i], core_peer)

    def o_group_core(i):
        return send(far_rows(6, i), far_rows(7, i), oyc_send.at[i], oyc_recv.at[i], core_peer)

    def kv_chip(s):
        return send(kv_v.at[s, own_rows], kv_v.at[s, own_rows], kx_send.at[s], kx_recv.at[s], chip_peer)

    def kv_core(s):
        return send(kv_v.at[s, own_rows], kv_v.at[s, own_rows], kc_send.at[s], kc_recv.at[s], core_peer)

    def kv_chip_core(s):
        return send(kv_v.at[s, chip_rows], kv_v.at[s, chip_rows], kxc_send.at[s], kxc_recv.at[s], core_peer)

    def kv_stores(s):
        outs = ((key_hbm, 0), (value_hbm, hd))
        return [pltpu.make_async_copy(kv_v.at[s, own_rows, pl.ds(at, hd)], ref.at[s], key_sem.at[s, i]) for i, (ref, at) in enumerate(outs)]

    def kv_send(s):
        kv_chip(s).start()
        kv_core(s).start()
        start(kv_stores(s))

    x_load(0).start()
    start(wkv + own_q)

    @pl.loop(1, num_batch)
    def _(s):
        x_load(s).start()

    enter(core_peer, chip_peer, group_peer)
    start([q_chip(i) for i in range(Q_PIECES)])
    start(q_core)
    start([o_chip(i) for i in range(O_PIECES)])
    start(o_core)

    gain = gain_ref[...].astype(F32)
    cos0, sin0 = cos0_ref[pl.ds(tp, 1), :], sin0_ref[pl.ds(tp, 1), :]
    cos_v[...] = cos_ref[...] * cos0 - sin_ref[...] * sin0
    sin_v[...] = sin_ref[...] * cos0 + cos_ref[...] * sin0
    for c in wkv + own_q:
        c.wait()

    def rope(x, cos, sin):
        a, c = x[:, :half], x[:, half:]
        return a * cos - c * sin, c * cos + a * sin

    def store_query(q, cos, sin, at, slot):
        lo, hi = rope(q, cos, sin)
        shape = q_v[at, slot, :, :half].shape
        q_v[at, slot, :, :half] = lo.astype(BF16).reshape(shape)
        q_v[at, slot, :, half:] = hi.astype(BF16).reshape(shape)

    @pl.loop(0, num_batch)
    def _(s):
        @pl.when(s == 5)
        def _():
            q_chip(0).wait_recv()
            start([q_group(0), q_chip_core(0)])

        @pl.when(s == num_batch - 1)
        def _():
            for i in range(1, Q_PIECES):
                q_chip(i).wait_recv()
                start([q_group(i), q_chip_core(i)])

        @pl.when(s > 0)
        def _():
            kv_send(s - 1)

        x_load(s).wait()
        xn = normalize(x_v[s].astype(F32), gain)
        x_v[s] = xn
        cos, sin = cos_v[...], sin_v[...]
        lo, hi = rope(dot(xn, wkv_v[0]), cos, sin)
        kv_v[s, own_rows, :half] = lo.astype(BF16)
        kv_v[s, own_rows, half:hd] = hi.astype(BF16)
        kv_v[s, own_rows, hd:] = dot(xn, wkv_v[1]).astype(BF16)
        for i in range(own_heads):
            store_query(dot(xn, w_v[i]), cos * hd**-0.5, sin * hd**-0.5, s, i)

    kv_send(num_batch - 1)

    group = 3

    @pl.loop(own_heads, heads)
    def _(slot):
        @pl.when(slot == 2)
        def _():
            wait_recv(q_core)

        @pl.when(slot == 3)
        def _():
            o_chip(0).wait_recv()
            start([o_group(0), o_chip_core(0)])

        @pl.when(slot == 5)
        def _():
            wait_recv([q_chip_core(i) for i in range(Q_PIECES)])
            o_chip(1).wait_recv()
            start([o_group(1), o_chip_core(1)])

        @pl.when(slot == 6)
        def _():
            for i in range(Q_PIECES):
                q_group(i).wait_recv()
                q_group_core(i).start()
            o_chip(2).wait_recv()
            start([o_group(2), o_chip_core(2)])

        @pl.when(slot == 7)
        def _():
            wait_recv([q_group_core(i) for i in range(Q_PIECES)])
            o_chip(3).wait_recv()
            start([o_group(3), o_chip_core(3)])

        @pl.loop(0, num_batch // group)
        def _(i):
            at = span(i, group)
            cos = jnp.concatenate([cos_v[...] * hd**-0.5] * group, axis=0)
            sin = jnp.concatenate([sin_v[...] * hd**-0.5] * group, axis=0)
            store_query(dot(x_v[at].reshape(group * rows, width), w_v[slot]), cos, sin, at, slot)

    for copies in ([q_group(i) for i in range(Q_PIECES)], [q_chip_core(i) for i in range(Q_PIECES)], [q_group_core(i) for i in range(Q_PIECES)]):
        wait_send(copies)
    for n in range(heads):
        own_o(n).start()

    @pl.loop(0, num_batch)
    def _(s):
        x_load(s).start()

    kv_chip(0).wait_recv()
    kv_chip_core(0).start()
    for i in range(O_PIECES):
        o_group(i).wait_recv()
        o_group_core(i).start()
    wait_recv(o_core + [o_chip_core(i) for i in range(O_PIECES)] + [o_group_core(i) for i in range(O_PIECES)])
    for n in range(heads):
        far_o(n).start()

    tail = 128
    col = lax.broadcasted_iota(jnp.int32, (rows, tail), 1) + (seq - tail)
    row = lax.broadcasted_iota(jnp.int32, (rows, tail), 0) + tp * rows

    def score(s, p):
        return lax.dot_general(q_v[s, p], kv_v[s, :, :hd], (((1,), (1,)), ((), ())), preferred_element_type=F32)

    def probs(sc, allowed):
        sc = jnp.concatenate([sc[:, : seq - tail], jnp.where(allowed, sc[:, seq - tail :], MASK_FILL)], axis=1)
        p = jnp.exp(sc - jnp.max(sc, axis=-1, keepdims=True))
        return (p * (1.0 / jnp.sum(p, axis=-1, keepdims=True))).astype(BF16)

    def project(s, n):
        o = jnp.concatenate([q_v[s, j] for j in range(heads)], axis=1)
        at = span(n, hd)
        x_v[s, :, at] = (x_v[s, :, at].astype(F32) + dot(o, w_v[n]).astype(BF16).astype(F32)).astype(BF16)

    gain2 = gain2_ref[...].astype(F32)

    def norm_rows(s, slot, at):
        x2_v[slot, at, :] = normalize(x_v[s, at, :].astype(F32), gain2)

    def h1_store(s):
        return pltpu.make_async_copy(x_v.at[s], h1_hbm.at[s], out_sem.at[s])

    def x2_store(s, slot):
        return pltpu.make_async_copy(x2_v.at[slot], x2_hbm.at[s], x2_sem.at[slot])

    @pl.loop(0, num_batch)
    def _(s):
        x_load(s).wait()

    for n in range(heads):
        own_o(n).wait()
        far_o(n).wait()

    last = num_batch - 1

    @pl.loop(0, num_batch)
    def _(s):
        before = lax.rem(s + last, num_batch)
        earlier = lax.rem(s + last - 1, num_batch)
        slot = lax.rem(s, 2)
        @pl.when(s < last)
        def _():
            kv_chip(s + 1).wait_recv()
            kv_chip_core(s + 1).start()

        wait_recv([kv_core(s), kv_chip_core(s)])
        allowed = (col < vlen_ref[s]) & ((col < plen_ref[s]) | (col <= row))

        @pl.when(s >= 4)
        def _():
            x2_store(s - 4, slot).wait()

        sc = score(s, 0)
        for p in range(heads):
            ahead = score(s, p + 1) if p + 1 < heads else None
            project(before, p)
            if p < 6:
                norm_rows(earlier, slot, pl.ds(p * 48, 48))
            pr = probs(sc, allowed)
            q_v[s, p] = dot(pr, kv_v[s, :, hd:]).astype(BF16)
            sc = ahead

        @pl.when(s >= 1)
        def _():
            h1_store(s - 1).start()

        @pl.when(s >= 2)
        def _():
            x2_store(s - 2, slot).start()

        @pl.when(s == 1)
        def _():
            x_load(last).start()

    x_load(last).wait()
    for n in range(heads):
        project(last, n)
    h1_store(last).start()
    for s in (last - 1, last):
        slot = s % 2
        x2_store(s - 2, slot).wait()
        norm_rows(s, slot, slice(None))
        x2_store(s, slot).start()

    wait_send(q_core + o_core + [q_chip(i) for i in range(Q_PIECES)])
    for i in range(O_PIECES):
        wait_send([o_chip(i), o_group(i), o_chip_core(i), o_group_core(i)])

    @pl.loop(0, num_batch)
    def _(s):
        wait_send([kv_chip(s), kv_core(s), kv_chip_core(s)])
        for c in kv_stores(s):
            c.wait()
        h1_store(s).wait()

    for s in (last - 1, last):
        x2_store(s, s % 2).wait()


def attention(hidden, prefix_len, valid_len, norm_attn, norm_mlp, w_query, w_key, w_value, w_out, tp_size):
    num_batch, rows, width = hidden.shape
    hd = w_key.shape[1]
    own_heads = w_query.shape[1] // hd
    heads = own_heads * tp_size
    seq = rows * tp_size
    tables = rope_tables(rows, tp_size, hd)
    any_spec = pl.BlockSpec(memory_space=pl.ANY)
    smem = pl.BlockSpec(memory_space=pltpu.SMEM)
    vmem = pl.BlockSpec(memory_space=pltpu.VMEM)
    dma = pltpu.SemaphoreType.DMA
    shape = jax.ShapeDtypeStruct
    flops = 2 * num_batch * rows * (width * (2 * heads + 2) * hd + 2 * heads * hd * seq)
    out = pl.pallas_call(
        attention_kernel,
        in_specs=[smem, smem, vmem, vmem, any_spec, vmem, vmem, vmem, vmem] + [any_spec] * 4,
        out_specs=[any_spec] * 5,
        out_shape=[
            shape((num_batch, rows, width), BF16),
            shape((num_batch, rows, width), BF16),
            shape((num_batch, rows, hd), BF16),
            shape((num_batch, rows, hd), BF16),
            shape(((heads - own_heads) * hd, width), BF16),
        ],
        scratch_shapes=[
            pltpu.VMEM((num_batch, rows, width), BF16),
            pltpu.VMEM((num_batch, heads, rows, hd), BF16),
            pltpu.VMEM((num_batch, seq, 2 * hd), BF16),
            pltpu.VMEM((heads, width, hd), BF16),
            pltpu.VMEM((2, width, hd), BF16),
            pltpu.VMEM((rows, hd // 2), F32),
            pltpu.VMEM((rows, hd // 2), F32),
            pltpu.VMEM((2, rows, width), BF16),
            dma((num_batch,)),
            dma((2,)),
            dma((heads, 2)),
            dma((num_batch,)),
            dma((2,)),
            dma((num_batch, 2)),
        ]
        + [dma((own_heads,))] * 2
        + [dma((Q_PIECES,))] * 8
        + [dma((1,))] * 2
        + [dma((O_PIECES,))] * 8
        + [dma((num_batch,))] * 6,
        compiler_params=pltpu.CompilerParams(vmem_limit_bytes=VMEM_LIMIT, collective_id=1, has_side_effects=True),
        cost_estimate=pl.CostEstimate(flops=flops, bytes_accessed=num_batch * rows * width * 6, transcendentals=num_batch * rows * heads * seq),
        name="attention",
    )(prefix_len, valid_len, norm_attn, norm_mlp, hidden, *(jnp.asarray(t) for t in tables), w_query, w_key, w_value, w_out)
    return out[:4]


GELU_LINEAR = 0.7978845608028654
GELU_CUBIC = GELU_LINEAR * 0.044715


def expand(x_ref, wg_ref, wu_ref, act_ref):
    block = 256
    for n in range(0, act_ref.shape[1], block):
        at = slice(n, n + block)
        gate = dot(x_ref[...], wg_ref[:, at])
        up = dot(x_ref[...], wu_ref[:, at])
        t = jnp.tanh(gate * (GELU_CUBIC * (gate * gate) + GELU_LINEAR))
        act_ref[:, at] = ((0.5 * gate) * up * (1.0 + t)).astype(BF16)


def mlp_kernel(x_hbm, wg_hbm, wu_hbm, wd_hbm, out_hbm, pg_hbm, pu_hbm, pd_hbm, rg_hbm, ru_hbm, rd_hbm,
               x_v, acc_v, act_v, wg_v, wu_v, wd_v, load_sem, x_sem, out_sem,
               p_send, p_recv, a_send, a_recv, ac_send, ac_recv, b_send, b_recv, bc_send, bc_recv):
    rows, width = x_v.shape
    tile = act_v.shape[1]
    tiles = rows // tile
    unit = wg_v.shape[2]
    piece = unit // 2
    own = wg_hbm.shape[1] // unit
    pieces = own // 2 * 2
    groups, per_group = rg_hbm.shape[:2]
    steps = 2 * own + groups * per_group - 1
    dp, tp, chip_tp, core_peer, chip_peer, group_peer = peers()

    def piece_refs(group, j):
        at = pl.ds(pl.multiple_of(lax.rem(j, 2) * piece, piece), piece)
        return rg_hbm.at[group, j // 2, :, at], ru_hbm.at[group, j // 2, :, at], rd_hbm.at[group, j // 2, at, :]

    def own_copies():
        refs = ((wg_hbm, pg_hbm), (wu_hbm, pu_hbm), (wd_hbm, pd_hbm))
        return [send(src, dst, p_send.at[i], p_recv.at[i], core_peer) for i, (src, dst) in enumerate(refs)]

    def chip_copies(j):
        at = pl.ds(pl.multiple_of(dp * pieces * piece + j * piece, piece), piece)
        src = (wg_hbm.at[:, at], wu_hbm.at[:, at], wd_hbm.at[at, :])
        return [send(s, d, a_send.at[j, i], a_recv.at[j, i], chip_peer) for i, (s, d) in enumerate(zip(src, piece_refs(0, j)))]

    def relay(j, source, target, send_sems, recv_sems, peer):
        pairs = zip(piece_refs(source, j), piece_refs(target, j))
        return [send(s, d, send_sems.at[j, i], recv_sems.at[j, i], peer) for i, (s, d) in enumerate(pairs)]

    def core_a(j):
        return relay(j, 0, 1, ac_send, ac_recv, core_peer)

    def group_a(j):
        return relay(j, 0, 2, b_send, b_recv, group_peer)

    def core_b(j):
        return relay(j, 2, 3, bc_send, bc_recv, core_peer)

    def x_copy(m):
        at = span(m, tile)
        return pltpu.make_async_copy(x_hbm.at[at], x_v.at[at], x_sem.at[m])

    def load(src, slot):
        return [pltpu.make_async_copy(s, d.at[slot], load_sem.at[slot, i]) for i, (s, d) in enumerate(zip(src, (wg_v, wu_v, wd_v)))]

    def own_load(u, slot):
        at = pl.ds(pl.multiple_of(u * unit, unit), unit)
        return load((wg_hbm.at[:, at], wu_hbm.at[:, at], wd_hbm.at[at, :]), slot)

    def peer_load(u, slot):
        at = pl.ds(pl.multiple_of((u - own) * unit, unit), unit)
        return load((pg_hbm.at[:, at], pu_hbm.at[:, at], pd_hbm.at[at, :]), slot)

    def far_load(u, slot):
        i = u - 2 * own
        g = lax.rem(i, groups)
        p = i // groups
        return load((rg_hbm.at[g, p], ru_hbm.at[g, p], rd_hbm.at[g, p]), slot)

    for m in range(tiles):
        x_copy(m).start()
    start(own_load(0, 0))
    enter(core_peer, chip_peer, group_peer)
    start(own_copies())

    @pl.loop(0, pieces)
    def _(j):
        start(chip_copies(j))

    @pl.loop(0, rows // 96)
    def _(i):
        acc_v[span(i, 96), :] = jnp.zeros((96, width), F32)

    for m in range(tiles):
        x_copy(m).wait()

    def out_copy(m):
        at = span(m, tile)
        return pltpu.make_async_copy(x_v.at[at], out_hbm.at[at], out_sem.at[m])

    first_a, first_b, every = 4, 8, 3

    @pl.loop(0, steps)
    def _(s):
        slot = lax.rem(s, 2)

        @pl.when((s >= first_a) & (s < first_a + every * pieces) & (lax.rem(s - first_a + every, every) == 0))
        def _():
            j = (s - first_a) // every
            wait_recv(chip_copies(j))
            start(group_a(j))
            start(core_a(j))

        @pl.when((s >= first_b) & (s < first_b + every * pieces) & (lax.rem(s - first_b + 2 * every, every) == 0))
        def _():
            j = (s - first_b) // every
            wait_recv(group_a(j))
            start(core_b(j))

        u = s + 1

        @pl.when(u < own)
        def _():
            start(own_load(u, 1 - slot))

        @pl.when(u == own)
        def _():
            wait_recv(own_copies())

        @pl.when((u >= own) & (u < 2 * own))
        def _():
            start(peer_load(u, 1 - slot))

        @pl.when((u >= 2 * own) & (u < steps))
        def _():
            g = lax.rem(u - 2 * own, groups)
            p = (u - 2 * own) // groups

            @pl.when(g == 1)
            def _():
                for j in (2 * p, 2 * p + 1):
                    wait_recv(core_a(j))

            @pl.when(g == 3)
            def _():
                for j in (2 * p, 2 * p + 1):
                    wait_recv(core_b(j))

            start(far_load(u, 1 - slot))

        for c in own_load(0, slot):
            c.wait()

        for m in range(tiles):
            at = pl.ds(m * tile, tile)
            expand(x_v.at[at], wg_v.at[slot], wu_v.at[slot], act_v.at[m % 2])
            for n in range(0, width, unit):
                acc_v[at, n : n + unit] += dot(act_v[m % 2], wd_v[slot, :, n : n + unit])

    for m in range(tiles):

        @pl.loop(0, tile // 96)
        def _(i):
            at = span(m * (tile // 96) + i, 96)
            x_v[at, :] = acc_v[at, :].astype(BF16)

        out_copy(m).start()

    for j in (pieces - 2, pieces - 1):
        wait_recv(core_b(j))
    wait_send(own_copies())

    @pl.loop(0, pieces)
    def _(j):
        for copies in (chip_copies(j), group_a(j), core_a(j), core_b(j)):
            wait_send(copies)

    for m in range(tiles):
        out_copy(m).wait()


def mlp(x2, w_gate, w_up, w_down):
    rows, width = x2.shape
    ff = w_gate.shape[1]
    unit = 512
    tile = rows // 6
    far = ff // 2 // unit
    pieces = 2 * far
    shapes = [(rows, width), (width, ff), (width, ff), (ff, width), (4, far, width, unit), (4, far, width, unit), (4, far, unit, width)]
    any_spec = pl.BlockSpec(memory_space=pl.ANY)
    dma = pltpu.SemaphoreType.DMA
    out = pl.pallas_call(
        mlp_kernel,
        in_specs=[any_spec] * 4,
        out_specs=[any_spec] * 7,
        out_shape=[jax.ShapeDtypeStruct(s, BF16) for s in shapes],
        scratch_shapes=[
            pltpu.VMEM((rows, width), BF16),
            pltpu.VMEM((rows, width), F32),
            pltpu.VMEM((2, tile, unit), BF16),
            pltpu.VMEM((2, width, unit), BF16),
            pltpu.VMEM((2, width, unit), BF16),
            pltpu.VMEM((2, unit, width), BF16),
            dma((2, 3)),
            dma((rows // tile,)),
            dma((rows // tile,)),
            dma((3,)),
            dma((3,)),
        ]
        + [dma((pieces, 3))] * 8,
        compiler_params=pltpu.CompilerParams(vmem_limit_bytes=VMEM_LIMIT, collective_id=0, has_side_effects=True),
        cost_estimate=pl.CostEstimate(flops=2 * rows * width * ff * 3 * 4, bytes_accessed=4 * 3 * width * ff * 2, transcendentals=0),
        name="mlp",
    )(x2, w_gate, w_up, w_down)
    return out[0], out[4:]


def last_kernel(x_ref, part_ref, h_ref, wg_ref, wu_ref, wd_ref, key_hbm, value_hbm, out_ref, key_out, value_out, act_v, cache_v, sem):
    i = pl.program_id(0)
    pairs = ((key_hbm, key_out), (value_hbm, value_out))
    loads = [pltpu.make_async_copy(src, cache_v.at[n], sem.at[n]) for n, (src, _) in enumerate(pairs)]
    stores = [pltpu.make_async_copy(cache_v.at[n], dst, sem.at[n]) for n, (_, dst) in enumerate(pairs)]

    @pl.when(i == 0)
    def _():
        start(loads)

    @pl.when(i == 1)
    def _():
        for load, store in zip(loads, stores):
            load.wait()
            store.start()

    expand(x_ref, wg_ref.at[0, 0], wu_ref.at[0, 0], act_v)
    block = 512
    for n in range(0, out_ref.shape[1], block):
        at = slice(n, n + block)
        total = part_ref[:, at].astype(F32) + dot(act_v[...], wd_ref[0, 0, :, at])
        out_ref[:, at] = (h_ref[:, at].astype(F32) + total.astype(BF16).astype(F32)).astype(BF16)

    @pl.when(i == pl.num_programs(0) - 1)
    def _():
        for store in stores:
            store.wait()


def finish(x2, part, h1, far_weights, key, value):
    rows, width = x2.shape
    tile = rows // 6
    groups, per_group = far_weights[0].shape[:2]
    row_block = pl.BlockSpec((tile, width), lambda i: (i, 0))
    any_spec = pl.BlockSpec(memory_space=pl.ANY)

    def weight_block(w):
        return pl.BlockSpec((1, 1) + w.shape[2:], lambda i: (groups - 1, per_group - 1, 0, 0), pipeline_mode=pl.Buffered(1))

    unit = far_weights[0].shape[3]
    shape = jax.ShapeDtypeStruct
    return pl.pallas_call(
        last_kernel,
        grid=(rows // tile,),
        in_specs=[row_block] * 3 + [weight_block(w) for w in far_weights] + [any_spec] * 2,
        out_specs=[row_block, any_spec, any_spec],
        out_shape=[shape(x2.shape, BF16), shape(key.shape, BF16), shape(value.shape, BF16)],
        scratch_shapes=[pltpu.VMEM((tile, unit), BF16), pltpu.VMEM((2,) + key.shape, BF16), pltpu.SemaphoreType.DMA((2,))],
        compiler_params=pltpu.CompilerParams(dimension_semantics=("arbitrary",), vmem_limit_bytes=60 << 20),
        cost_estimate=pl.CostEstimate(flops=6 * rows * width * unit, bytes_accessed=8 * rows * width, transcendentals=0),
        name="finish",
    )(x2, part, h1, *far_weights, key, value)


def solution(mesh):
    tp_size = mesh.shape["tp"]
    row_spec = P("dp", "tp", None)
    arg_specs = (row_spec, P("dp"), P("dp"), P(), P(None, "tp"), P(), P(), P("tp", None), P(), P(None, "tp"), P(None, "tp"), P("tp", None))

    def local_layer(hidden, prefix_len, valid_len, norm_attn, w_query, w_key, w_value, w_out, norm_mlp, w_gate, w_up, w_down):
        h1, x2, key, value = attention(hidden, prefix_len, valid_len, norm_attn, norm_mlp, w_query, w_key, w_value, w_out, tp_size)
        flat = (-1, hidden.shape[-1])
        x2 = x2.reshape(flat)
        part, far_weights = mlp(x2, w_gate, w_up, w_down)
        out, key, value = finish(x2, part, h1.reshape(flat), far_weights, key, value)
        return out.reshape(hidden.shape), key, value

    return jax.shard_map(local_layer, mesh=mesh, in_specs=arg_specs, out_specs=(row_spec, row_spec, row_spec), check_vma=False)
```

```python
import functools

import jax
import jax.numpy as jnp
import numpy as np
from jax import lax
from jax.experimental import pallas as pl
from jax.experimental.pallas import tpu as pltpu
from jax.sharding import PartitionSpec as P

NORM_EPS = 1e-6
ROPE_BASE = 10000.0
MASK_FILL = -1e30
F32 = jnp.float32
BF16 = jnp.bfloat16
MESH = pl.DeviceIdType.MESH
VMEM_LIMIT = 67043328


def rope_tables(rows, blocks, head_dim):
    inv_freq = ROPE_BASE ** (-2.0 * np.arange(head_dim // 2) / head_dim)
    angles = np.arange(rows)[:, None] * inv_freq[None, :]
    starts = np.arange(blocks)[:, None] * rows * inv_freq[None, :]
    return tuple(f(a).astype(np.float32) for a in (angles, starts) for f in (np.cos, np.sin))


def normalize(rows, gain):
    inv = lax.rsqrt(jnp.mean(rows * rows, axis=-1, keepdims=True) + NORM_EPS)
    return (rows * inv * (1.0 + gain)).astype(BF16)


def dot(a, b):
    return jnp.dot(a, b, preferred_element_type=F32)


def span(index, size):
    return pl.ds(pl.multiple_of(index * size, size), size)


def start(copies):
    for c in copies:
        c.start()


def wait_recv(copies):
    for c in copies:
        c.wait_recv()


def wait_send(copies):
    for c in copies:
        c.wait_send()


def send(src, dst, send_sem, recv_sem, peer):
    return pltpu.make_async_remote_copy(src_ref=src, dst_ref=dst, send_sem=send_sem, recv_sem=recv_sem, device_id=peer, device_id_type=MESH)


def peers():
    dp = lax.axis_index("dp")
    tp = lax.axis_index("tp")
    core_tp = tp + 1 - 2 * lax.rem(tp, 2)
    chip_tp = lax.rem(tp + 2, 4)
    return dp, tp, chip_tp, {"tp": core_tp}, {"tp": chip_tp}, {"dp": 1 - dp}


def enter(*others):
    barrier = pltpu.get_barrier_semaphore()
    for peer in others:
        pl.semaphore_signal(barrier, inc=1, device_id=peer, device_id_type=MESH)
    pl.semaphore_wait(barrier, len(others))


Q_PIECES = 2
O_PIECES = 4


GELU_LINEAR = 0.7978845608028654
GELU_CUBIC = GELU_LINEAR * 0.044715


def expand(x_ref, gate_refs, up_refs, act_ref):
    for i, (gate_ref, up_ref) in enumerate(zip(gate_refs, up_refs)):
        block = gate_ref.shape[1]
        at = slice(i * block, (i + 1) * block)
        gate = dot(x_ref[...], gate_ref[...])
        up = dot(x_ref[...], up_ref[...])
        t = jnp.tanh(gate * (GELU_CUBIC * (gate * gate) + GELU_LINEAR))
        act_ref[:, at] = ((0.5 * gate) * up * (1.0 + t)).astype(BF16)


def layer_kernel(plen_ref, vlen_ref, gain_ref, gain2_ref, h_hbm, cos_ref, sin_ref, cos0_ref, sin0_ref, wq_hbm, wk_hbm, wv_hbm, wo_hbm, wg_hbm, wu_hbm, wd_hbm,
                 part_hbm, h1_hbm, x2_hbm, key_hbm, value_hbm, wo_far, pg_hbm, pu_hbm, pd_hbm, rg_hbm, ru_hbm, rd_hbm,
                 x_v, w_v, wd_v, act_v,
                 x_sem, wkv_sem, w_sem, out_sem, x2_sem, key_sem, load_sem, part_sem,
                 qc_send, qc_recv, qx_send, qx_recv, qy_send, qy_recv, qxc_send, qxc_recv, qyc_send, qyc_recv,
                 oc_send, oc_recv, ox_send, ox_recv, oy_send, oy_recv, oxc_send, oxc_recv, oyc_send, oyc_recv,
                 kx_send, kx_recv, kc_send, kc_recv, kxc_send, kxc_recv,
                 p_send, p_recv, a_send, a_recv, ac_send, ac_recv, b_send, b_recv, bc_send, bc_recv):
    num_batch, rows, width = h_hbm.shape
    total = num_batch * rows
    hd = wk_hbm.shape[1]
    half = hd // 2
    own_heads = wq_hbm.shape[1] // hd
    heads = w_v.shape[0]
    seq = rows * heads // own_heads
    tile = act_v.shape[1]
    tiles = total // tile
    unit = act_v.shape[2]
    piece = unit // 2
    own = wg_hbm.shape[1] // unit
    groups, pieces = rg_hbm.shape[:2]
    steps = 2 * own + groups * pieces // 2 - 1
    dp, tp, chip_tp, core_peer, chip_peer, group_peer = peers()
    own_rows = span(tp, rows)
    chip_rows = span(chip_tp, rows)

    def piece_refs(group, j):
        return rg_hbm.at[group, j], ru_hbm.at[group, j], rd_hbm.at[group, j]

    def own_copies():
        refs = ((wg_hbm, pg_hbm), (wu_hbm, pu_hbm), (wd_hbm, pd_hbm))
        return [send(src, dst, p_send.at[i], p_recv.at[i], core_peer) for i, (src, dst) in enumerate(refs)]

    def chip_copies(j):
        at = pl.ds(pl.multiple_of(dp * pieces * piece + j * piece, piece), piece)
        src = (wg_hbm.at[:, at], wu_hbm.at[:, at], wd_hbm.at[at, :])
        return [send(s, d, a_send.at[j, i], a_recv.at[j, i], chip_peer) for i, (s, d) in enumerate(zip(src, piece_refs(0, j)))]

    def relay(j, source, target, send_sems, recv_sems, peer):
        pairs = zip(piece_refs(source, j), piece_refs(target, j))
        return [send(s, d, send_sems.at[j, i], recv_sems.at[j, i], peer) for i, (s, d) in enumerate(pairs)]

    def core_a(j):
        return relay(j, 0, 1, ac_send, ac_recv, core_peer)

    def group_a(j):
        return relay(j, 0, 2, b_send, b_recv, group_peer)

    def core_b(j):
        return relay(j, 2, 3, bc_send, bc_recv, core_peer)

    def load(srcs, slot):
        dsts = [w_v.at[4 * slot + i] for i in range(4)] + [wd_v.at[slot, pl.ds(i * piece, piece)] for i in range(2)]
        return [pltpu.make_async_copy(src, dst, load_sem.at[slot, i]) for i, (src, dst) in enumerate(zip(srcs, dsts))]

    def near_load(refs, u, slot):
        ats = [pl.ds(pl.multiple_of(u * unit + i * piece, piece), piece) for i in range(2)]
        return load([refs[0].at[:, at] for at in ats] + [refs[1].at[:, at] for at in ats] + [refs[2].at[at] for at in ats], slot)

    def own_load(u, slot):
        return near_load((wg_hbm, wu_hbm, wd_hbm), u, slot)

    def peer_load(u, slot):
        return near_load((pg_hbm, pu_hbm, pd_hbm), u - own, slot)

    def far_load(u, slot):
        g = lax.rem(u - 2 * own, groups)
        p = (u - 2 * own) // groups
        return load([ref.at[g, 2 * p + i] for ref in (rg_hbm, ru_hbm, rd_hbm) for i in range(2)], slot)

    def h1_store(s):
        return pltpu.make_async_copy(x_v.at[span(s, rows)], h1_hbm.at[s], out_sem.at[s])

    def x2_store(s):
        return pltpu.make_async_copy(x_v.at[span(s, rows)], x2_hbm.at[s], x2_sem.at[s])

    def attend(q_v, kv_v, wkv_v, cos_v, sin_v):

        wkv = [pltpu.make_async_copy(w, wkv_v.at[i], wkv_sem.at[i]) for i, w in enumerate((wk_hbm, wv_hbm))]
        own_q = [pltpu.make_async_copy(wq_hbm.at[:, pl.ds(i * hd, hd)], w_v.at[i], w_sem.at[i, 0]) for i in range(own_heads)]

        def x_load(s):
            return pltpu.make_async_copy(h_hbm.at[s], x_v.at[span(s, rows)], x_sem.at[s])

        def own_o(n):
            return pltpu.make_async_copy(wo_hbm.at[:, pl.ds(n * hd, hd)], w_v.at[n, pl.ds(0, own_heads * hd)], w_sem.at[n, 0])

        def far_o(n):
            size = (heads - own_heads) * hd
            return pltpu.make_async_copy(wo_far.at[:, pl.ds(n * hd, hd)], w_v.at[n, pl.ds(own_heads * hd, size)], w_sem.at[n, 1])

        q_core = [send(wq_hbm.at[:, pl.ds(i * hd, hd)], w_v.at[own_heads + i], qc_send.at[i], qc_recv.at[i], core_peer) for i in range(own_heads)]
        q_rows = width // Q_PIECES

        def q_chip(i):
            return send(wq_hbm.at[pl.ds(i * q_rows, q_rows), span(dp, hd)], w_v.at[4, pl.ds(i * q_rows, q_rows)], qx_send.at[i], qx_recv.at[i], chip_peer)

        def q_move(src, dst, i, send_sem, recv_sem, peer):
            at = pl.ds(i * q_rows, q_rows)
            return send(w_v.at[src, at], w_v.at[dst, at], send_sem.at[i], recv_sem.at[i], peer)

        def q_group(i):
            return q_move(4, 6, i, qy_send, qy_recv, group_peer)

        def q_chip_core(i):
            return q_move(4, 5, i, qxc_send, qxc_recv, core_peer)

        def q_group_core(i):
            return q_move(6, 7, i, qyc_send, qyc_recv, core_peer)

        own_width = own_heads * hd
        o_rows = hd // O_PIECES
        o_core = [send(wo_hbm, wo_far.at[pl.ds(0, own_width)], oc_send.at[0], oc_recv.at[0], core_peer)]

        def far_rows(slot, i):
            return wo_far.at[pl.ds((slot - own_heads) * hd + i * o_rows, o_rows)]

        def o_chip(i):
            src = wo_hbm.at[pl.ds(pl.multiple_of(dp * hd + i * o_rows, o_rows), o_rows)]
            return send(src, far_rows(4, i), ox_send.at[i], ox_recv.at[i], chip_peer)

        def o_group(i):
            return send(far_rows(4, i), far_rows(6, i), oy_send.at[i], oy_recv.at[i], group_peer)

        def o_chip_core(i):
            return send(far_rows(4, i), far_rows(5, i), oxc_send.at[i], oxc_recv.at[i], core_peer)

        def o_group_core(i):
            return send(far_rows(6, i), far_rows(7, i), oyc_send.at[i], oyc_recv.at[i], core_peer)

        def kv_chip(s):
            return send(kv_v.at[s, own_rows], kv_v.at[s, own_rows], kx_send.at[s], kx_recv.at[s], chip_peer)

        def kv_core(s):
            return send(kv_v.at[s, own_rows], kv_v.at[s, own_rows], kc_send.at[s], kc_recv.at[s], core_peer)

        def kv_chip_core(s):
            return send(kv_v.at[s, chip_rows], kv_v.at[s, chip_rows], kxc_send.at[s], kxc_recv.at[s], core_peer)

        def kv_stores(s):
            outs = ((key_hbm, 0), (value_hbm, hd))
            return [pltpu.make_async_copy(kv_v.at[s, own_rows, pl.ds(at, hd)], ref.at[s], key_sem.at[s, i]) for i, (ref, at) in enumerate(outs)]

        def kv_send(s):
            kv_chip(s).start()
            kv_core(s).start()
            start(kv_stores(s))

        x_load(0).start()
        start(wkv + own_q)

        @pl.loop(1, num_batch)
        def _(s):
            x_load(s).start()

        enter(core_peer, chip_peer, group_peer)
        start([q_chip(i) for i in range(Q_PIECES)])
        start(q_core)
        start([o_chip(i) for i in range(O_PIECES)])
        start(o_core)

        gain = gain_ref[...].astype(F32)
        cos0, sin0 = cos0_ref[pl.ds(tp, 1), :], sin0_ref[pl.ds(tp, 1), :]
        cos_v[...] = cos_ref[...] * cos0 - sin_ref[...] * sin0
        sin_v[...] = sin_ref[...] * cos0 + cos_ref[...] * sin0
        for c in wkv + own_q:
            c.wait()

        def rope(x, cos, sin):
            a, c = x[:, :half], x[:, half:]
            return a * cos - c * sin, c * cos + a * sin

        def store_query(q, cos, sin, at, slot):
            lo, hi = rope(q, cos, sin)
            shape = q_v[at, slot, :, :half].shape
            q_v[at, slot, :, :half] = lo.astype(BF16).reshape(shape)
            q_v[at, slot, :, half:] = hi.astype(BF16).reshape(shape)

        @pl.loop(0, num_batch)
        def _(s):
            @pl.when(s == 5)
            def _():
                q_chip(0).wait_recv()
                start([q_group(0), q_chip_core(0)])

            @pl.when(s == num_batch - 1)
            def _():
                for i in range(1, Q_PIECES):
                    q_chip(i).wait_recv()
                    start([q_group(i), q_chip_core(i)])

            @pl.when(s > 0)
            def _():
                kv_send(s - 1)

            x_load(s).wait()
            at = span(s, rows)
            xn = normalize(x_v[at, :].astype(F32), gain)
            x_v[at, :] = xn
            cos, sin = cos_v[...], sin_v[...]
            lo, hi = rope(dot(xn, wkv_v[0]), cos, sin)
            kv_v[s, own_rows, :half] = lo.astype(BF16)
            kv_v[s, own_rows, half:hd] = hi.astype(BF16)
            kv_v[s, own_rows, hd:] = dot(xn, wkv_v[1]).astype(BF16)
            for i in range(own_heads):
                store_query(dot(xn, w_v[i]), cos * hd**-0.5, sin * hd**-0.5, s, i)

        kv_send(num_batch - 1)

        group = 3

        @pl.loop(own_heads, heads)
        def _(slot):
            @pl.when(slot == 2)
            def _():
                wait_recv(q_core)

            @pl.when(slot == 3)
            def _():
                o_chip(0).wait_recv()
                start([o_group(0), o_chip_core(0)])

            @pl.when(slot == 5)
            def _():
                wait_recv([q_chip_core(i) for i in range(Q_PIECES)])
                o_chip(1).wait_recv()
                start([o_group(1), o_chip_core(1)])

            @pl.when(slot == 6)
            def _():
                for i in range(Q_PIECES):
                    q_group(i).wait_recv()
                    q_group_core(i).start()
                o_chip(2).wait_recv()
                start([o_group(2), o_chip_core(2)])

            @pl.when(slot == 7)
            def _():
                wait_recv([q_group_core(i) for i in range(Q_PIECES)])
                o_chip(3).wait_recv()
                start([o_group(3), o_chip_core(3)])

            @pl.loop(0, num_batch // group)
            def _(i):
                at = span(i, group)
                cos = jnp.concatenate([cos_v[...] * hd**-0.5] * group, axis=0)
                sin = jnp.concatenate([sin_v[...] * hd**-0.5] * group, axis=0)
                store_query(dot(x_v[span(i, group * rows), :], w_v[slot]), cos, sin, at, slot)

        for copies in ([q_group(i) for i in range(Q_PIECES)], [q_chip_core(i) for i in range(Q_PIECES)], [q_group_core(i) for i in range(Q_PIECES)]):
            wait_send(copies)
        for n in range(heads):
            own_o(n).start()

        @pl.loop(0, num_batch)
        def _(s):
            x_load(s).start()

        kv_chip(0).wait_recv()
        kv_chip_core(0).start()
        for i in range(O_PIECES):
            o_group(i).wait_recv()
            o_group_core(i).start()
        wait_recv(o_core + [o_chip_core(i) for i in range(O_PIECES)] + [o_group_core(i) for i in range(O_PIECES)])
        for n in range(heads):
            far_o(n).start()

        tail = 128
        col = lax.broadcasted_iota(jnp.int32, (rows, tail), 1) + (seq - tail)
        row = lax.broadcasted_iota(jnp.int32, (rows, tail), 0) + tp * rows

        def score(s, p):
            return lax.dot_general(q_v[s, p], kv_v[s, :, :hd], (((1,), (1,)), ((), ())), preferred_element_type=F32)

        def probs(sc, allowed):
            sc = jnp.concatenate([sc[:, : seq - tail], jnp.where(allowed, sc[:, seq - tail :], MASK_FILL)], axis=1)
            p = jnp.exp(sc - jnp.max(sc, axis=-1, keepdims=True))
            return (p * (1.0 / jnp.sum(p, axis=-1, keepdims=True))).astype(BF16)

        def project(s, n):
            o = jnp.concatenate([q_v[s, j] for j in range(heads)], axis=1)
            at = span(s, rows), slice(n * hd, (n + 1) * hd)
            x_v[at] = (x_v[at].astype(F32) + dot(o, w_v[n]).astype(BF16).astype(F32)).astype(BF16)

        gain2 = gain2_ref[...].astype(F32)

        def norm_rows(s, first, size):
            at = pl.ds(pl.multiple_of(s * rows + first, 16), size)
            x_v[at, :] = normalize(x_v[at, :].astype(F32), gain2)

        @pl.loop(0, num_batch)
        def _(s):
            x_load(s).wait()

        for n in range(heads):
            own_o(n).wait()
            far_o(n).wait()

        last = num_batch - 1

        @pl.loop(0, num_batch)
        def _(s):
            before = lax.rem(s + last, num_batch)
            earlier = lax.rem(s + last - 2, num_batch)

            @pl.when(s < last)
            def _():
                kv_chip(s + 1).wait_recv()
                kv_chip_core(s + 1).start()

            @pl.when(s == last)
            def _():
                start(own_copies())

                @pl.loop(0, pieces)
                def _(j):
                    start(chip_copies(j))

            @pl.when(s == last - 2)
            def _():
                for i in range(last - 2, last + 1):
                    x_load(i).wait()

            @pl.when(s >= 3)
            def _():
                h1_store(s - 3).wait()

            wait_recv([kv_core(s), kv_chip_core(s)])
            allowed = (col < vlen_ref[s]) & ((col < plen_ref[s]) | (col <= row))
            sc = score(s, 0)
            for p in range(heads):
                ahead = score(s, p + 1) if p + 1 < heads else None
                project(before, p)
                if p < 6:
                    norm_rows(earlier, p * 48, 48)
                pr = probs(sc, allowed)
                q_v[s, p] = dot(pr, kv_v[s, :, hd:]).astype(BF16)
                sc = ahead

            @pl.when(s >= 1)
            def _():
                h1_store(s - 1).start()

            @pl.when(s >= 3)
            def _():
                x2_store(s - 3).start()

            @pl.when(s == 2)
            def _():
                for i in range(last - 2, last + 1):
                    x_load(i).start()

        for n in range(heads):
            project(last, n)
            if n == 3:
                start(own_load(0, 0))
        h1_store(last).start()
        for s in range(last - 2, last + 1):
            h1_store(s).wait()
            norm_rows(s, 0, rows)
            x2_store(s).start()

        wait_send(q_core + o_core + [q_chip(i) for i in range(Q_PIECES)])
        for i in range(O_PIECES):
            wait_send([o_chip(i), o_group(i), o_chip_core(i), o_group_core(i)])

        @pl.loop(0, num_batch)
        def _(s):
            wait_send([kv_chip(s), kv_core(s), kv_chip_core(s)])
            for c in kv_stores(s):
                c.wait()

    def feed_forward(acc_v):
        @pl.loop(0, total // 96)
        def _(i):
            acc_v[span(i, 96), :] = jnp.zeros((96, width), F32)

        def out_copy(m):
            at = span(m, tile)
            return pltpu.make_async_copy(x_v.at[at], part_hbm.at[at], part_sem.at[m])

        first_a, first_b, every = 3, 7, 3

        @pl.loop(0, steps)
        def _(s):
            slot = lax.rem(s, 2)

            @pl.when((s >= first_a) & (s < first_a + every * pieces) & (lax.rem(s, every) == first_a % every))
            def _():
                j = (s - first_a) // every
                wait_recv(chip_copies(j))
                start(group_a(j))
                start(core_a(j))

            @pl.when((s >= first_b) & (s < first_b + every * pieces) & (lax.rem(s, every) == first_b % every))
            def _():
                j = (s - first_b) // every
                wait_recv(group_a(j))
                start(core_b(j))

            u = s + 1

            @pl.when(u < own)
            def _():
                start(own_load(u, 1 - slot))

            @pl.when(u == own)
            def _():
                wait_recv(own_copies())

            @pl.when((u >= own) & (u < 2 * own))
            def _():
                start(peer_load(u, 1 - slot))

            @pl.when((u >= 2 * own) & (u < steps))
            def _():
                g = lax.rem(u - 2 * own, groups)
                p = (u - 2 * own) // groups

                @pl.when(g == 1)
                def _():
                    for j in (2 * p, 2 * p + 1):
                        wait_recv(core_a(j))

                @pl.when(g == 3)
                def _():
                    for j in (2 * p, 2 * p + 1):
                        wait_recv(core_b(j))

                start(far_load(u, 1 - slot))

            for c in own_load(0, slot):
                c.wait()

            gate = [w_v.at[4 * slot + i] for i in range(2)]
            up = [w_v.at[4 * slot + 2 + i] for i in range(2)]
            for m in range(tiles):
                at = pl.ds(m * tile, tile)
                expand(x_v.at[at], gate, up, act_v.at[m % 2])
                for n in range(0, width, unit):
                    acc_v[at, n : n + unit] += dot(act_v[m % 2], wd_v[slot, :, n : n + unit])

        @pl.loop(0, num_batch)
        def _(s):
            x2_store(s).wait()

        for m in range(tiles):

            @pl.loop(0, tile // 96)
            def _(i):
                at = span(m * (tile // 96) + i, 96)
                x_v[at, :] = acc_v[at, :].astype(BF16)

            out_copy(m).start()

        for j in (pieces - 2, pieces - 1):
            wait_recv(core_b(j))
        wait_send(own_copies())

        @pl.loop(0, pieces)
        def _(j):
            for copies in (chip_copies(j), group_a(j), core_a(j), core_b(j)):
                wait_send(copies)

        for m in range(tiles):
            out_copy(m).wait()

    pl.run_scoped(
        attend,
        pltpu.VMEM((num_batch, heads, rows, hd), BF16),
        pltpu.VMEM((num_batch, seq, 2 * hd), BF16),
        pltpu.VMEM((2, width, hd), BF16),
        pltpu.VMEM((rows, half), F32),
        pltpu.VMEM((rows, half), F32),
    )
    pl.run_scoped(feed_forward, pltpu.VMEM((total, width), F32))


def layer(hidden, prefix_len, valid_len, norm_attn, norm_mlp, w_query, w_key, w_value, w_out, w_gate, w_up, w_down, tp_size):
    num_batch, rows, width = hidden.shape
    total = num_batch * rows
    hd = w_key.shape[1]
    own_heads = w_query.shape[1] // hd
    heads = own_heads * tp_size
    seq = rows * tp_size
    ff = w_gate.shape[1]
    piece = 256
    pieces = ff // 2 // piece
    tile = total // 6
    tables = rope_tables(rows, tp_size, hd)
    any_spec = pl.BlockSpec(memory_space=pl.ANY)
    smem = pl.BlockSpec(memory_space=pltpu.SMEM)
    vmem = pl.BlockSpec(memory_space=pltpu.VMEM)
    dma = pltpu.SemaphoreType.DMA
    outs = [(total, width), (num_batch, rows, width), (num_batch, rows, width), (num_batch, rows, hd), (num_batch, rows, hd)]
    outs += [((heads - own_heads) * hd, width), (width, ff), (width, ff), (ff, width)]
    outs += [(4, pieces, width, piece), (4, pieces, width, piece), (4, pieces, piece, width)]
    flops = 2 * total * (width * (2 * heads + 2) * hd + 2 * heads * hd * seq + 3 * width * ff * tp_size)
    out = pl.pallas_call(
        layer_kernel,
        in_specs=[smem, smem, vmem, vmem, any_spec, vmem, vmem, vmem, vmem] + [any_spec] * 7,
        out_specs=[any_spec] * len(outs),
        out_shape=[jax.ShapeDtypeStruct(s, BF16) for s in outs],
        scratch_shapes=[
            pltpu.VMEM((total, width), BF16),
            pltpu.VMEM((heads, width, hd), BF16),
            pltpu.VMEM((2, 2 * piece, width), BF16),
            pltpu.VMEM((2, tile, 2 * piece), BF16),
            dma((num_batch,)),
            dma((2,)),
            dma((heads, 2)),
            dma((num_batch,)),
            dma((num_batch,)),
            dma((num_batch, 2)),
            dma((2, 6)),
            dma((total // tile,)),
        ]
        + [dma((own_heads,))] * 2
        + [dma((Q_PIECES,))] * 8
        + [dma((1,))] * 2
        + [dma((O_PIECES,))] * 8
        + [dma((num_batch,))] * 6
        + [dma((3,))] * 2
        + [dma((pieces, 3))] * 8,
        compiler_params=pltpu.CompilerParams(vmem_limit_bytes=VMEM_LIMIT, collective_id=0, has_side_effects=True),
        cost_estimate=pl.CostEstimate(flops=flops, bytes_accessed=8 * 3 * width * ff, transcendentals=total * (heads * seq + ff * tp_size)),
        name="layer",
    )(prefix_len, valid_len, norm_attn, norm_mlp, hidden, *(jnp.asarray(t) for t in tables), w_query, w_key, w_value, w_out, w_gate, w_up, w_down)
    return out[:5], out[9:]


def last_kernel(x_ref, part_ref, h_ref, wg_ref, wu_ref, wd_ref, key_hbm, value_hbm, out_ref, key_out, value_out, act_v, cache_v, sem):
    i = pl.program_id(0)
    pairs = ((key_hbm, key_out), (value_hbm, value_out))
    loads = [pltpu.make_async_copy(src, cache_v.at[n], sem.at[n]) for n, (src, _) in enumerate(pairs)]
    stores = [pltpu.make_async_copy(cache_v.at[n], dst, sem.at[n]) for n, (_, dst) in enumerate(pairs)]

    @pl.when(i == 0)
    def _():
        start(loads)

    @pl.when(i == 1)
    def _():
        for load, store in zip(loads, stores):
            load.wait()
            store.start()

    expand(x_ref, [wg_ref.at[0, n] for n in range(2)], [wu_ref.at[0, n] for n in range(2)], act_v)
    block = 512
    for n in range(0, out_ref.shape[1], block):
        at = slice(n, n + block)
        total = part_ref[:, at].astype(F32) + dot(act_v[...], wd_ref[0, :, :, at].reshape(act_v.shape[1], block))
        out_ref[:, at] = (h_ref[:, at].astype(F32) + total.astype(BF16).astype(F32)).astype(BF16)

    @pl.when(i == pl.num_programs(0) - 1)
    def _():
        for store in stores:
            store.wait()


def finish(x2, part, h1, far_weights, key, value):
    rows, width = x2.shape
    tile = rows // 6
    groups, pieces = far_weights[0].shape[:2]
    row_block = pl.BlockSpec((tile, width), lambda i: (i, 0))
    any_spec = pl.BlockSpec(memory_space=pl.ANY)

    def weight_block(w):
        return pl.BlockSpec((1, 2) + w.shape[2:], lambda i: (groups - 1, pieces // 2 - 1, 0, 0), pipeline_mode=pl.Buffered(1))

    unit = 2 * far_weights[0].shape[3]
    shape = jax.ShapeDtypeStruct
    return pl.pallas_call(
        last_kernel,
        grid=(rows // tile,),
        in_specs=[row_block] * 3 + [weight_block(w) for w in far_weights] + [any_spec] * 2,
        out_specs=[row_block, any_spec, any_spec],
        out_shape=[shape(x2.shape, BF16), shape(key.shape, BF16), shape(value.shape, BF16)],
        scratch_shapes=[pltpu.VMEM((tile, unit), BF16), pltpu.VMEM((2,) + key.shape, BF16), pltpu.SemaphoreType.DMA((2,))],
        compiler_params=pltpu.CompilerParams(dimension_semantics=("arbitrary",), vmem_limit_bytes=60 << 20),
        cost_estimate=pl.CostEstimate(flops=6 * rows * width * unit, bytes_accessed=8 * rows * width, transcendentals=0),
        name="finish",
    )(x2, part, h1, *far_weights, key, value)


def solution(mesh):
    tp_size = mesh.shape["tp"]
    row_spec = P("dp", "tp", None)
    arg_specs = (row_spec, P("dp"), P("dp"), P(), P(None, "tp"), P(), P(), P("tp", None), P(), P(None, "tp"), P(None, "tp"), P("tp", None))

    def local_layer(hidden, prefix_len, valid_len, norm_attn, w_query, w_key, w_value, w_out, norm_mlp, w_gate, w_up, w_down):
        (part, h1, x2, key, value), far_weights = layer(hidden, prefix_len, valid_len, norm_attn, norm_mlp, w_query, w_key, w_value, w_out, w_gate, w_up, w_down, tp_size)
        flat = (-1, hidden.shape[-1])
        out, key, value = finish(x2.reshape(flat), part, h1.reshape(flat), far_weights, key, value)
        return out.reshape(hidden.shape), key, value

    return jax.shard_map(local_layer, mesh=mesh, in_specs=arg_specs, out_specs=(row_spec, row_spec, row_spec), check_vma=False)
```

```python
import functools

import jax
import jax.numpy as jnp
import numpy as np
from jax import lax
from jax.experimental import pallas as pl
from jax.experimental.pallas import tpu as pltpu
from jax.sharding import PartitionSpec as P

NORM_EPS = 1e-6
ROPE_BASE = 10000.0
MASK_FILL = -1e30
F32 = jnp.float32
BF16 = jnp.bfloat16
MESH = pl.DeviceIdType.MESH
VMEM_LIMIT = 67043328


def rope_tables(rows, blocks, head_dim):
    inv_freq = ROPE_BASE ** (-2.0 * np.arange(head_dim // 2) / head_dim)
    angles = np.arange(rows)[:, None] * inv_freq[None, :]
    starts = np.arange(blocks)[:, None] * rows * inv_freq[None, :]
    return tuple(f(a).astype(np.float32) for a in (angles, starts) for f in (np.cos, np.sin))


def normalize(rows, gain):
    inv = lax.rsqrt(jnp.mean(rows * rows, axis=-1, keepdims=True) + NORM_EPS)
    return (rows * inv * (1.0 + gain)).astype(BF16)


def dot(a, b):
    return jnp.dot(a, b, preferred_element_type=F32)


def span(index, size):
    return pl.ds(pl.multiple_of(index * size, size), size)


def start(copies):
    for c in copies:
        c.start()


def wait_recv(copies):
    for c in copies:
        c.wait_recv()


def wait_send(copies):
    for c in copies:
        c.wait_send()


def send(src, dst, send_sem, recv_sem, peer):
    return pltpu.make_async_remote_copy(src_ref=src, dst_ref=dst, send_sem=send_sem, recv_sem=recv_sem, device_id=peer, device_id_type=MESH)


def peers():
    dp = lax.axis_index("dp")
    tp = lax.axis_index("tp")
    core_tp = tp + 1 - 2 * lax.rem(tp, 2)
    chip_tp = lax.rem(tp + 2, 4)
    return dp, tp, chip_tp, {"tp": core_tp}, {"tp": chip_tp}, {"dp": 1 - dp}


def enter(*others):
    barrier = pltpu.get_barrier_semaphore()
    for peer in others:
        pl.semaphore_signal(barrier, inc=1, device_id=peer, device_id_type=MESH)
    pl.semaphore_wait(barrier, len(others))


Q_PIECES = 2
O_PIECES = 4


GELU_LINEAR = 0.7978845608028654
GELU_CUBIC = GELU_LINEAR * 0.044715


def expand(x_ref, gate_refs, up_refs, act_ref):
    for i, (gate_ref, up_ref) in enumerate(zip(gate_refs, up_refs)):
        block = gate_ref.shape[1]
        at = slice(i * block, (i + 1) * block)
        gate = dot(x_ref[...], gate_ref[...])
        up = dot(x_ref[...], up_ref[...])
        t = jnp.tanh(gate * (GELU_CUBIC * (gate * gate) + GELU_LINEAR))
        act_ref[:, at] = ((0.5 * gate) * up * (1.0 + t)).astype(BF16)


def layer_kernel(plen_ref, vlen_ref, gain_ref, gain2_ref, h_hbm, cos_ref, sin_ref, cos0_ref, sin0_ref, wq_hbm, wk_hbm, wv_hbm, wo_hbm, wg_hbm, wu_hbm, wd_hbm,
                 part_hbm, h1_hbm, x2_hbm, key_hbm, value_hbm, wo_far, pg_hbm, pu_hbm, pd_hbm, rg_hbm, ru_hbm, rd_hbm,
                 x_v, w_v, wd_v, act_v,
                 x_sem, wkv_sem, w_sem, out_sem, x2_sem, key_sem, load_sem, part_sem,
                 qc_send, qc_recv, qx_send, qx_recv, qy_send, qy_recv, qxc_send, qxc_recv, qyc_send, qyc_recv,
                 oc_send, oc_recv, ox_send, ox_recv, oy_send, oy_recv, oxc_send, oxc_recv, oyc_send, oyc_recv,
                 kx_send, kx_recv, kc_send, kc_recv, kxc_send, kxc_recv,
                 p_send, p_recv, a_send, a_recv, ac_send, ac_recv, b_send, b_recv, bc_send, bc_recv):
    num_batch, rows, width = h_hbm.shape
    total = num_batch * rows
    hd = wk_hbm.shape[1]
    half = hd // 2
    own_heads = wq_hbm.shape[1] // hd
    heads = w_v.shape[0]
    seq = rows * heads // own_heads
    tile = act_v.shape[1]
    tiles = total // tile
    unit = act_v.shape[2]
    piece = unit // 2
    own = wg_hbm.shape[1] // unit
    groups, pieces = rg_hbm.shape[:2]
    steps = 2 * own + groups * pieces // 2 - 1
    dp, tp, chip_tp, core_peer, chip_peer, group_peer = peers()
    own_rows = span(tp, rows)
    chip_rows = span(chip_tp, rows)

    def piece_refs(group, j):
        return rg_hbm.at[group, j], ru_hbm.at[group, j], rd_hbm.at[group, j]

    def own_copies():
        refs = ((wg_hbm, pg_hbm), (wu_hbm, pu_hbm), (wd_hbm, pd_hbm))
        return [send(src, dst, p_send.at[i], p_recv.at[i], core_peer) for i, (src, dst) in enumerate(refs)]

    def chip_copies(j):
        at = pl.ds(pl.multiple_of(dp * pieces * piece + j * piece, piece), piece)
        src = (wg_hbm.at[:, at], wu_hbm.at[:, at], wd_hbm.at[at, :])
        return [send(s, d, a_send.at[j, i], a_recv.at[j, i], chip_peer) for i, (s, d) in enumerate(zip(src, piece_refs(0, j)))]

    def relay(j, source, target, send_sems, recv_sems, peer):
        pairs = zip(piece_refs(source, j), piece_refs(target, j))
        return [send(s, d, send_sems.at[j, i], recv_sems.at[j, i], peer) for i, (s, d) in enumerate(pairs)]

    def core_a(j):
        return relay(j, 0, 1, ac_send, ac_recv, core_peer)

    def group_a(j):
        return relay(j, 0, 2, b_send, b_recv, group_peer)

    def core_b(j):
        return relay(j, 2, 3, bc_send, bc_recv, core_peer)

    def load(srcs, slot):
        dsts = [w_v.at[4 * slot + i] for i in range(4)] + [wd_v.at[slot, pl.ds(i * piece, piece)] for i in range(2)]
        return [pltpu.make_async_copy(src, dst, load_sem.at[slot, i]) for i, (src, dst) in enumerate(zip(srcs, dsts))]

    def near_load(refs, u, slot):
        ats = [pl.ds(pl.multiple_of(u * unit + i * piece, piece), piece) for i in range(2)]
        return load([refs[0].at[:, at] for at in ats] + [refs[1].at[:, at] for at in ats] + [refs[2].at[at] for at in ats], slot)

    def own_load(u, slot):
        return near_load((wg_hbm, wu_hbm, wd_hbm), u, slot)

    def peer_load(u, slot):
        return near_load((pg_hbm, pu_hbm, pd_hbm), u - own, slot)

    def far_load(u, slot):
        g = lax.rem(u - 2 * own, groups)
        p = (u - 2 * own) // groups
        return load([ref.at[g, 2 * p + i] for ref in (rg_hbm, ru_hbm, rd_hbm) for i in range(2)], slot)

    def h1_store(s):
        return pltpu.make_async_copy(x_v.at[span(s, rows)], h1_hbm.at[s], out_sem.at[s])

    def x2_store(s):
        return pltpu.make_async_copy(x_v.at[span(s, rows)], x2_hbm.at[s], x2_sem.at[s])

    def attend(q_v, kv_v, wkv_v, cos_v, sin_v):

        wkv = [pltpu.make_async_copy(w, wkv_v.at[i], wkv_sem.at[i]) for i, w in enumerate((wk_hbm, wv_hbm))]
        own_q = [pltpu.make_async_copy(wq_hbm.at[:, pl.ds(i * hd, hd)], w_v.at[i], w_sem.at[i, 0]) for i in range(own_heads)]

        def x_load(s):
            return pltpu.make_async_copy(h_hbm.at[s], x_v.at[span(s, rows)], x_sem.at[s])

        def own_o(n):
            return pltpu.make_async_copy(wo_hbm.at[:, pl.ds(n * hd, hd)], w_v.at[n, pl.ds(0, own_heads * hd)], w_sem.at[n, 0])

        def far_o(n):
            size = (heads - own_heads) * hd
            return pltpu.make_async_copy(wo_far.at[:, pl.ds(n * hd, hd)], w_v.at[n, pl.ds(own_heads * hd, size)], w_sem.at[n, 1])

        q_core = [send(wq_hbm.at[:, pl.ds(i * hd, hd)], w_v.at[own_heads + i], qc_send.at[i], qc_recv.at[i], core_peer) for i in range(own_heads)]
        q_rows = width // Q_PIECES

        def q_chip(i):
            return send(wq_hbm.at[pl.ds(i * q_rows, q_rows), span(dp, hd)], w_v.at[4, pl.ds(i * q_rows, q_rows)], qx_send.at[i], qx_recv.at[i], chip_peer)

        def q_move(src, dst, i, send_sem, recv_sem, peer):
            at = pl.ds(i * q_rows, q_rows)
            return send(w_v.at[src, at], w_v.at[dst, at], send_sem.at[i], recv_sem.at[i], peer)

        def q_group(i):
            return q_move(4, 6, i, qy_send, qy_recv, group_peer)

        def q_chip_core(i):
            return q_move(4, 5, i, qxc_send, qxc_recv, core_peer)

        def q_group_core(i):
            return q_move(6, 7, i, qyc_send, qyc_recv, core_peer)

        own_width = own_heads * hd
        o_rows = hd // O_PIECES
        o_core = [send(wo_hbm, wo_far.at[pl.ds(0, own_width)], oc_send.at[0], oc_recv.at[0], core_peer)]

        def far_rows(slot, i):
            return wo_far.at[pl.ds((slot - own_heads) * hd + i * o_rows, o_rows)]

        def o_chip(i):
            src = wo_hbm.at[pl.ds(pl.multiple_of(dp * hd + i * o_rows, o_rows), o_rows)]
            return send(src, far_rows(4, i), ox_send.at[i], ox_recv.at[i], chip_peer)

        def o_group(i):
            return send(far_rows(4, i), far_rows(6, i), oy_send.at[i], oy_recv.at[i], group_peer)

        def o_chip_core(i):
            return send(far_rows(4, i), far_rows(5, i), oxc_send.at[i], oxc_recv.at[i], core_peer)

        def o_group_core(i):
            return send(far_rows(6, i), far_rows(7, i), oyc_send.at[i], oyc_recv.at[i], core_peer)

        def kv_chip(s):
            return send(kv_v.at[s, own_rows], kv_v.at[s, own_rows], kx_send.at[s], kx_recv.at[s], chip_peer)

        def kv_core(s):
            return send(kv_v.at[s, own_rows], kv_v.at[s, own_rows], kc_send.at[s], kc_recv.at[s], core_peer)

        def kv_chip_core(s):
            return send(kv_v.at[s, chip_rows], kv_v.at[s, chip_rows], kxc_send.at[s], kxc_recv.at[s], core_peer)

        def kv_stores(s):
            outs = ((key_hbm, 0), (value_hbm, hd))
            return [pltpu.make_async_copy(kv_v.at[s, own_rows, pl.ds(at, hd)], ref.at[s], key_sem.at[s, i]) for i, (ref, at) in enumerate(outs)]

        def kv_send(s):
            kv_chip(s).start()
            kv_core(s).start()
            start(kv_stores(s))

        x_load(0).start()
        start(wkv + own_q)

        @pl.loop(1, num_batch)
        def _(s):
            x_load(s).start()

        enter(core_peer, chip_peer, group_peer)
        start([q_chip(i) for i in range(Q_PIECES)])
        start(q_core)
        start([o_chip(i) for i in range(O_PIECES)])
        start(o_core)

        gain = gain_ref[...].astype(F32)
        cos0, sin0 = cos0_ref[pl.ds(tp, 1), :], sin0_ref[pl.ds(tp, 1), :]
        cos_v[...] = cos_ref[...] * cos0 - sin_ref[...] * sin0
        sin_v[...] = sin_ref[...] * cos0 + cos_ref[...] * sin0
        for c in wkv + own_q:
            c.wait()

        def rope(x, cos, sin):
            a, c = x[:, :half], x[:, half:]
            return a * cos - c * sin, c * cos + a * sin

        def store_query(q, cos, sin, at, slot):
            lo, hi = rope(q, cos, sin)
            shape = q_v[at, slot, :, :half].shape
            q_v[at, slot, :, :half] = lo.astype(BF16).reshape(shape)
            q_v[at, slot, :, half:] = hi.astype(BF16).reshape(shape)

        @pl.loop(0, num_batch)
        def _(s):
            @pl.when(s == 5)
            def _():
                q_chip(0).wait_recv()
                start([q_group(0), q_chip_core(0)])

            @pl.when(s == num_batch - 1)
            def _():
                for i in range(1, Q_PIECES):
                    q_chip(i).wait_recv()
                    start([q_group(i), q_chip_core(i)])

            @pl.when(s > 0)
            def _():
                kv_send(s - 1)

            x_load(s).wait()
            at = span(s, rows)
            xn = normalize(x_v[at, :].astype(F32), gain)
            x_v[at, :] = xn
            cos, sin = cos_v[...], sin_v[...]
            lo, hi = rope(dot(xn, wkv_v[0]), cos, sin)
            kv_v[s, own_rows, :half] = lo.astype(BF16)
            kv_v[s, own_rows, half:hd] = hi.astype(BF16)
            kv_v[s, own_rows, hd:] = dot(xn, wkv_v[1]).astype(BF16)
            for i in range(own_heads):
                store_query(dot(xn, w_v[i]), cos * hd**-0.5, sin * hd**-0.5, s, i)

        kv_send(num_batch - 1)

        group = 3

        @pl.loop(own_heads, heads)
        def _(slot):
            @pl.when(slot == 2)
            def _():
                wait_recv(q_core)

            @pl.when(slot == 3)
            def _():
                o_chip(0).wait_recv()
                start([o_group(0), o_chip_core(0)])

            @pl.when(slot == 5)
            def _():
                wait_recv([q_chip_core(i) for i in range(Q_PIECES)])
                o_chip(1).wait_recv()
                start([o_group(1), o_chip_core(1)])

            @pl.when(slot == 6)
            def _():
                for i in range(Q_PIECES):
                    q_group(i).wait_recv()
                    q_group_core(i).start()
                o_chip(2).wait_recv()
                start([o_group(2), o_chip_core(2)])

            @pl.when(slot == 7)
            def _():
                wait_recv([q_group_core(i) for i in range(Q_PIECES)])
                o_chip(3).wait_recv()
                start([o_group(3), o_chip_core(3)])

            @pl.loop(0, num_batch // group)
            def _(i):
                at = span(i, group)
                cos = jnp.concatenate([cos_v[...] * hd**-0.5] * group, axis=0)
                sin = jnp.concatenate([sin_v[...] * hd**-0.5] * group, axis=0)
                store_query(dot(x_v[span(i, group * rows), :], w_v[slot]), cos, sin, at, slot)

        for copies in ([q_group(i) for i in range(Q_PIECES)], [q_chip_core(i) for i in range(Q_PIECES)], [q_group_core(i) for i in range(Q_PIECES)]):
            wait_send(copies)
        for n in range(heads):
            own_o(n).start()

        @pl.loop(0, num_batch)
        def _(s):
            x_load(s).start()

        kv_chip(0).wait_recv()
        kv_chip_core(0).start()
        for i in range(O_PIECES):
            o_group(i).wait_recv()
            o_group_core(i).start()
        wait_recv(o_core + [o_chip_core(i) for i in range(O_PIECES)] + [o_group_core(i) for i in range(O_PIECES)])
        for n in range(heads):
            far_o(n).start()

        tail = 128
        col = lax.broadcasted_iota(jnp.int32, (rows, tail), 1) + (seq - tail)
        row = lax.broadcasted_iota(jnp.int32, (rows, tail), 0) + tp * rows

        def score(s, p):
            return lax.dot_general(q_v[s, p], kv_v[s, :, :hd], (((1,), (1,)), ((), ())), preferred_element_type=F32)

        def probs(sc, allowed):
            sc = jnp.concatenate([sc[:, : seq - tail], jnp.where(allowed, sc[:, seq - tail :], MASK_FILL)], axis=1)
            p = jnp.exp(sc - jnp.max(sc, axis=-1, keepdims=True))
            return (p * (1.0 / jnp.sum(p, axis=-1, keepdims=True))).astype(BF16)

        def project(s, n):
            o = jnp.concatenate([q_v[s, j] for j in range(heads)], axis=1)
            at = span(s, rows), span(n, hd)
            x_v[at] = (x_v[at].astype(F32) + dot(o, w_v[n]).astype(BF16).astype(F32)).astype(BF16)

        gain2 = gain2_ref[...].astype(F32)

        def norm_rows(s, first, size):
            at = pl.ds(pl.multiple_of(s * rows + first, 16), size)
            x_v[at, :] = normalize(x_v[at, :].astype(F32), gain2)

        @pl.loop(0, num_batch)
        def _(s):
            x_load(s).wait()

        for n in range(heads):
            own_o(n).wait()
            far_o(n).wait()

        last = num_batch - 1

        @pl.loop(0, num_batch)
        def _(s):
            before = lax.rem(s + last, num_batch)
            earlier = lax.rem(s + last - 2, num_batch)

            @pl.when(s < last)
            def _():
                kv_chip(s + 1).wait_recv()
                kv_chip_core(s + 1).start()

            @pl.when(s == last)
            def _():
                start(own_copies())

                @pl.loop(0, pieces)
                def _(j):
                    start(chip_copies(j))

            @pl.when(s == last - 2)
            def _():
                for i in range(last - 2, last + 1):
                    x_load(i).wait()

            @pl.when(s >= 3)
            def _():
                h1_store(s - 3).wait()

            wait_recv([kv_core(s), kv_chip_core(s)])
            allowed = (col < vlen_ref[s]) & ((col < plen_ref[s]) | (col <= row))
            sc = score(s, 0)
            for p in range(heads):
                ahead = score(s, p + 1) if p + 1 < heads else None
                project(before, p)
                if p < 6:
                    norm_rows(earlier, p * 48, 48)
                pr = probs(sc, allowed)
                q_v[s, p] = dot(pr, kv_v[s, :, hd:]).astype(BF16)
                sc = ahead

            @pl.when(s >= 1)
            def _():
                h1_store(s - 1).start()

            @pl.when(s >= 3)
            def _():
                x2_store(s - 3).start()

            @pl.when(s == 2)
            def _():
                for i in range(last - 2, last + 1):
                    x_load(i).start()

        @pl.loop(0, heads // 2)
        def _(i):
            @pl.when(i == heads // 4)
            def _():
                start(own_load(0, 0))

            project(last, 2 * i)
            project(last, 2 * i + 1)

        h1_store(last).start()
        for s in range(last - 2, last + 1):
            h1_store(s).wait()
            norm_rows(s, 0, rows)
            x2_store(s).start()

        wait_send(q_core + o_core + [q_chip(i) for i in range(Q_PIECES)])
        for i in range(O_PIECES):
            wait_send([o_chip(i), o_group(i), o_chip_core(i), o_group_core(i)])

        @pl.loop(0, num_batch)
        def _(s):
            wait_send([kv_chip(s), kv_core(s), kv_chip_core(s)])
            for c in kv_stores(s):
                c.wait()

    def feed_forward(acc_v):
        @pl.loop(0, total // 96)
        def _(i):
            acc_v[span(i, 96), :] = jnp.zeros((96, width), F32)

        def out_copy(m):
            at = span(m, tile)
            return pltpu.make_async_copy(x_v.at[at], part_hbm.at[at], part_sem.at[m])

        first_a, first_b, every = 4, 8, 3

        @pl.loop(0, steps)
        def _(s):
            slot = lax.rem(s, 2)

            @pl.when((s >= first_a) & (s < first_a + every * pieces) & (lax.rem(s, every) == first_a % every))
            def _():
                j = (s - first_a) // every
                wait_recv(chip_copies(j))
                start(group_a(j))
                start(core_a(j))

            @pl.when((s >= first_b) & (s < first_b + every * pieces) & (lax.rem(s, every) == first_b % every))
            def _():
                j = (s - first_b) // every
                wait_recv(group_a(j))
                start(core_b(j))

            u = s + 1

            @pl.when(u < own)
            def _():
                start(own_load(u, 1 - slot))

            @pl.when(u == own)
            def _():
                wait_recv(own_copies())

            @pl.when((u >= own) & (u < 2 * own))
            def _():
                start(peer_load(u, 1 - slot))

            @pl.when((u >= 2 * own) & (u < steps))
            def _():
                g = lax.rem(u - 2 * own, groups)
                p = (u - 2 * own) // groups

                @pl.when(g == 1)
                def _():
                    for j in (2 * p, 2 * p + 1):
                        wait_recv(core_a(j))

                @pl.when(g == 3)
                def _():
                    for j in (2 * p, 2 * p + 1):
                        wait_recv(core_b(j))

                start(far_load(u, 1 - slot))

            for c in own_load(0, slot):
                c.wait()

            gate = [w_v.at[4 * slot + i] for i in range(2)]
            up = [w_v.at[4 * slot + 2 + i] for i in range(2)]
            for m in range(tiles):
                at = pl.ds(m * tile, tile)
                expand(x_v.at[at], gate, up, act_v.at[m % 2])
                for n in range(0, width, unit):
                    acc_v[at, n : n + unit] += dot(act_v[m % 2], wd_v[slot, :, n : n + unit])

        @pl.loop(0, num_batch)
        def _(s):
            x2_store(s).wait()

        for m in range(tiles):

            @pl.loop(0, tile // 96)
            def _(i):
                at = span(m * (tile // 96) + i, 96)
                x_v[at, :] = acc_v[at, :].astype(BF16)

            out_copy(m).start()

        for j in (pieces - 2, pieces - 1):
            wait_recv(core_b(j))
        wait_send(own_copies())

        @pl.loop(0, pieces)
        def _(j):
            for copies in (chip_copies(j), group_a(j), core_a(j), core_b(j)):
                wait_send(copies)

        for m in range(tiles):
            out_copy(m).wait()

    pl.run_scoped(
        attend,
        pltpu.VMEM((num_batch, heads, rows, hd), BF16),
        pltpu.VMEM((num_batch, seq, 2 * hd), BF16),
        pltpu.VMEM((2, width, hd), BF16),
        pltpu.VMEM((rows, half), F32),
        pltpu.VMEM((rows, half), F32),
    )
    pl.run_scoped(feed_forward, pltpu.VMEM((total, width), F32))


def layer(hidden, prefix_len, valid_len, norm_attn, norm_mlp, w_query, w_key, w_value, w_out, w_gate, w_up, w_down, tp_size):
    num_batch, rows, width = hidden.shape
    total = num_batch * rows
    hd = w_key.shape[1]
    own_heads = w_query.shape[1] // hd
    heads = own_heads * tp_size
    seq = rows * tp_size
    ff = w_gate.shape[1]
    piece = 256
    pieces = ff // 2 // piece
    tile = total // 6
    tables = rope_tables(rows, tp_size, hd)
    any_spec = pl.BlockSpec(memory_space=pl.ANY)
    smem = pl.BlockSpec(memory_space=pltpu.SMEM)
    vmem = pl.BlockSpec(memory_space=pltpu.VMEM)
    dma = pltpu.SemaphoreType.DMA
    outs = [(total, width), (num_batch, rows, width), (num_batch, rows, width), (num_batch, rows, hd), (num_batch, rows, hd)]
    outs += [((heads - own_heads) * hd, width), (width, ff), (width, ff), (ff, width)]
    outs += [(4, pieces, width, piece), (4, pieces, width, piece), (4, pieces, piece, width)]
    flops = 2 * total * (width * (2 * heads + 2) * hd + 2 * heads * hd * seq + 3 * width * ff * tp_size)
    out = pl.pallas_call(
        layer_kernel,
        in_specs=[smem, smem, vmem, vmem, any_spec, vmem, vmem, vmem, vmem] + [any_spec] * 7,
        out_specs=[any_spec] * len(outs),
        out_shape=[jax.ShapeDtypeStruct(s, BF16) for s in outs],
        scratch_shapes=[
            pltpu.VMEM((total, width), BF16),
            pltpu.VMEM((heads, width, hd), BF16),
            pltpu.VMEM((2, 2 * piece, width), BF16),
            pltpu.VMEM((2, tile, 2 * piece), BF16),
            dma((num_batch,)),
            dma((2,)),
            dma((heads, 2)),
            dma((num_batch,)),
            dma((num_batch,)),
            dma((num_batch, 2)),
            dma((2, 6)),
            dma((total // tile,)),
        ]
        + [dma((own_heads,))] * 2
        + [dma((Q_PIECES,))] * 8
        + [dma((1,))] * 2
        + [dma((O_PIECES,))] * 8
        + [dma((num_batch,))] * 6
        + [dma((3,))] * 2
        + [dma((pieces, 3))] * 8,
        compiler_params=pltpu.CompilerParams(vmem_limit_bytes=VMEM_LIMIT, collective_id=0, has_side_effects=True),
        cost_estimate=pl.CostEstimate(flops=flops, bytes_accessed=8 * 3 * width * ff, transcendentals=total * (heads * seq + ff * tp_size)),
        name="layer",
    )(prefix_len, valid_len, norm_attn, norm_mlp, hidden, *(jnp.asarray(t) for t in tables), w_query, w_key, w_value, w_out, w_gate, w_up, w_down)
    return out[:5], out[9:]


def last_kernel(x_hbm, part_hbm, h_hbm, wg_hbm, wu_hbm, wd_hbm, key_hbm, value_hbm, out_hbm, key_out, value_out,
                x_v, part_v, h_v, wg_v, wu_v, wd_v, act_v, cache_v, w_sem, row_sem, out_sem, cache_sem):
    rows, width = x_v.shape
    tile, unit = act_v.shape
    tiles = rows // tile
    groups, pieces = wg_hbm.shape[:2]
    pairs = ((key_hbm, key_out), (value_hbm, value_out))
    loads = [pltpu.make_async_copy(src, cache_v.at[n], cache_sem.at[n]) for n, (src, _) in enumerate(pairs)]
    stores = [pltpu.make_async_copy(cache_v.at[n], dst, cache_sem.at[n]) for n, (_, dst) in enumerate(pairs)]
    weights = [
        pltpu.make_async_copy(src.at[groups - 1, pl.ds(pieces - 2, 2)], dst, w_sem.at[n])
        for n, (src, dst) in enumerate(((wg_hbm, wg_v), (wu_hbm, wu_v), (wd_hbm, wd_v)))
    ]

    def row_load(m, n):
        at = span(m, tile)
        src, dst = ((x_hbm, x_v), (part_hbm, part_v), (h_hbm, h_v))[n]
        return pltpu.make_async_copy(src.at[at], dst.at[at], row_sem.at[m, n])

    def out_store(m):
        at = span(m, tile)
        return pltpu.make_async_copy(h_v.at[at], out_hbm.at[at], out_sem.at[m])

    row_load(0, 0).start()
    start(weights[:2])
    row_load(0, 0).wait()
    for c in weights[:2]:
        c.wait()
    weights[2].start()
    start([row_load(0, n) for n in (1, 2)])

    @pl.loop(1, tiles)
    def _(m):
        start([row_load(m, n) for n in range(3)])

    start(loads)

    @pl.loop(0, tiles)
    def _(m):
        at = span(m, tile)

        @pl.when(m == tiles // 2)
        def _():
            for load, store in zip(loads, stores):
                load.wait()
                store.start()

        @pl.when(m > 0)
        def _():
            for n in range(3):
                row_load(m, n).wait()

        expand(x_v.at[at], [wg_v.at[n] for n in range(2)], [wu_v.at[n] for n in range(2)], act_v)

        @pl.when(m == 0)
        def _():
            weights[2].wait()
            for n in (1, 2):
                row_load(0, n).wait()

        block = 512
        for n in range(0, width, block):
            cols = slice(n, n + block)
            total = part_v[at, cols].astype(F32) + dot(act_v[...], wd_v[:, :, cols].reshape(unit, block))
            h_v[at, cols] = (h_v[at, cols].astype(F32) + total.astype(BF16).astype(F32)).astype(BF16)
        out_store(m).start()

    for store in stores:
        store.wait()
    for m in range(tiles):
        out_store(m).wait()


def finish(x2, part, h1, far_weights, key, value):
    rows, width = x2.shape
    tile = rows // 4
    piece = far_weights[0].shape[3]
    any_spec = pl.BlockSpec(memory_space=pl.ANY)
    dma = pltpu.SemaphoreType.DMA
    shape = jax.ShapeDtypeStruct
    return pl.pallas_call(
        last_kernel,
        in_specs=[any_spec] * 8,
        out_specs=[any_spec] * 3,
        out_shape=[shape(x2.shape, BF16), shape(key.shape, BF16), shape(value.shape, BF16)],
        scratch_shapes=[pltpu.VMEM((rows, width), BF16)] * 3
        + [
            pltpu.VMEM((2, width, piece), BF16),
            pltpu.VMEM((2, width, piece), BF16),
            pltpu.VMEM((2, piece, width), BF16),
            pltpu.VMEM((tile, 2 * piece), BF16),
            pltpu.VMEM((2,) + key.shape, BF16),
            dma((3,)),
            dma((rows // tile, 3)),
            dma((rows // tile,)),
            dma((2,)),
        ],
        compiler_params=pltpu.CompilerParams(vmem_limit_bytes=VMEM_LIMIT),
        cost_estimate=pl.CostEstimate(flops=12 * rows * width * piece, bytes_accessed=8 * rows * width, transcendentals=0),
        name="finish",
    )(x2, part, h1, *far_weights, key, value)


def solution(mesh):
    tp_size = mesh.shape["tp"]
    row_spec = P("dp", "tp", None)
    arg_specs = (row_spec, P("dp"), P("dp"), P(), P(None, "tp"), P(), P(), P("tp", None), P(), P(None, "tp"), P(None, "tp"), P("tp", None))

    def local_layer(hidden, prefix_len, valid_len, norm_attn, w_query, w_key, w_value, w_out, norm_mlp, w_gate, w_up, w_down):
        (part, h1, x2, key, value), far_weights = layer(hidden, prefix_len, valid_len, norm_attn, norm_mlp, w_query, w_key, w_value, w_out, w_gate, w_up, w_down, tp_size)
        flat = (-1, hidden.shape[-1])
        out, key, value = finish(x2.reshape(flat), part, h1.reshape(flat), far_weights, key, value)
        return out.reshape(hidden.shape), key, value

    return jax.shard_map(local_layer, mesh=mesh, in_specs=arg_specs, out_specs=(row_spec, row_spec, row_spec), check_vma=False)
```

```python
import functools

import jax
import jax.numpy as jnp
import numpy as np
from jax import lax
from jax.experimental import pallas as pl
from jax.experimental.pallas import tpu as pltpu
from jax.sharding import PartitionSpec as P

NORM_EPS = 1e-6
ROPE_BASE = 10000.0
MASK_FILL = -1e30
F32 = jnp.float32
BF16 = jnp.bfloat16
MESH = pl.DeviceIdType.MESH
VMEM_LIMIT = 67043328


def rope_tables(seq, block, head_dim):
    inv_freq = ROPE_BASE ** (-2.0 * np.arange(head_dim // 2) / head_dim)
    angles = np.arange(block)[:, None] * inv_freq[None, :]
    starts = np.arange(0, seq, block)[:, None] * inv_freq[None, :]
    return tuple(f(a).astype(np.float32) for a in (angles, starts) for f in (np.cos, np.sin))


def normalize(rows, gain):
    inv = lax.rsqrt(jnp.mean(rows * rows, axis=-1, keepdims=True) + NORM_EPS)
    return (rows * inv * (1.0 + gain)).astype(BF16)


def dot(a, b):
    return jnp.dot(a, b, preferred_element_type=F32)


def span(index, size):
    return pl.ds(pl.multiple_of(index * size, size), size)


def start(copies):
    for c in copies:
        c.start()


def wait_recv(copies):
    for c in copies:
        c.wait_recv()


def wait_send(copies):
    for c in copies:
        c.wait_send()


def send(src, dst, send_sem, recv_sem, peer):
    return pltpu.make_async_remote_copy(src_ref=src, dst_ref=dst, send_sem=send_sem, recv_sem=recv_sem, device_id=peer, device_id_type=MESH)


def peers():
    dp = lax.axis_index("dp")
    tp = lax.axis_index("tp")
    core_tp = tp + 1 - 2 * lax.rem(tp, 2)
    chip_tp = lax.rem(tp + 2, 4)
    return dp, tp, chip_tp, {"tp": core_tp}, {"tp": chip_tp}, {"dp": 1 - dp}


def enter(*others):
    barrier = pltpu.get_barrier_semaphore()
    for peer in others:
        pl.semaphore_signal(barrier, inc=1, device_id=peer, device_id_type=MESH)
    pl.semaphore_wait(barrier, len(others))


Q_PIECES = 2
O_PIECES = 4
LAST_UNITS = 1


def attention_kernel(plen_ref, vlen_ref, gain_ref, gain2_ref, h_hbm, cos_ref, sin_ref, cos0_ref, sin0_ref, wq_hbm, wk_hbm, wv_hbm, wo_hbm,
                     h1_hbm, x2_hbm, key_hbm, value_hbm, wo_far,
                     x_v, q_v, kv_v, w_v, wkv_v, cos_v, sin_v, x2_v,
                     x_sem, wkv_sem, w_sem, out_sem, x2_sem, key_sem,
                     qc_send, qc_recv, qx_send, qx_recv, qy_send, qy_recv, qxc_send, qxc_recv, qyc_send, qyc_recv,
                     oc_send, oc_recv, ox_send, ox_recv, oy_send, oy_recv, oxc_send, oxc_recv, oyc_send, oyc_recv,
                     kx_send, kx_recv, kc_send, kc_recv, kxc_send, kxc_recv):
    num_batch, rows, width = x_v.shape
    heads, hd = q_v.shape[1], q_v.shape[3]
    seq = kv_v.shape[1]
    own_heads = wq_hbm.shape[1] // hd
    half = hd // 2
    dp, tp, chip_tp, core_peer, chip_peer, group_peer = peers()
    own_rows = span(tp, rows)
    chip_rows = span(chip_tp, rows)

    wkv = [pltpu.make_async_copy(w, wkv_v.at[i], wkv_sem.at[i]) for i, w in enumerate((wk_hbm, wv_hbm))]
    own_q = [pltpu.make_async_copy(wq_hbm.at[:, pl.ds(i * hd, hd)], w_v.at[i], w_sem.at[i, 0]) for i in range(own_heads)]

    def x_load(s):
        return pltpu.make_async_copy(h_hbm.at[s], x_v.at[s], x_sem.at[s])

    def own_o(n):
        return pltpu.make_async_copy(wo_hbm.at[:, pl.ds(n * hd, hd)], w_v.at[n, pl.ds(0, own_heads * hd)], w_sem.at[n, 0])

    def far_o(n):
        size = (heads - own_heads) * hd
        return pltpu.make_async_copy(wo_far.at[:, pl.ds(n * hd, hd)], w_v.at[n, pl.ds(own_heads * hd, size)], w_sem.at[n, 1])

    q_core = [send(wq_hbm.at[:, pl.ds(i * hd, hd)], w_v.at[own_heads + i], qc_send.at[i], qc_recv.at[i], core_peer) for i in range(own_heads)]
    q_rows = width // Q_PIECES

    def q_chip(i):
        return send(wq_hbm.at[pl.ds(i * q_rows, q_rows), span(dp, hd)], w_v.at[4, pl.ds(i * q_rows, q_rows)], qx_send.at[i], qx_recv.at[i], chip_peer)

    def q_move(src, dst, i, send_sem, recv_sem, peer):
        at = pl.ds(i * q_rows, q_rows)
        return send(w_v.at[src, at], w_v.at[dst, at], send_sem.at[i], recv_sem.at[i], peer)

    def q_group(i):
        return q_move(4, 6, i, qy_send, qy_recv, group_peer)

    def q_chip_core(i):
        return q_move(4, 5, i, qxc_send, qxc_recv, core_peer)

    def q_group_core(i):
        return q_move(6, 7, i, qyc_send, qyc_recv, core_peer)

    own_width = own_heads * hd
    o_rows = hd // O_PIECES
    o_core = [send(wo_hbm, wo_far.at[pl.ds(0, own_width)], oc_send.at[0], oc_recv.at[0], core_peer)]

    def far_rows(slot, i):
        return wo_far.at[pl.ds((slot - own_heads) * hd + i * o_rows, o_rows)]

    def o_chip(i):
        src = wo_hbm.at[pl.ds(pl.multiple_of(dp * hd + i * o_rows, o_rows), o_rows)]
        return send(src, far_rows(4, i), ox_send.at[i], ox_recv.at[i], chip_peer)

    def o_group(i):
        return send(far_rows(4, i), far_rows(6, i), oy_send.at[i], oy_recv.at[i], group_peer)

    def o_chip_core(i):
        return send(far_rows(4, i), far_rows(5, i), oxc_send.at[i], oxc_recv.at[i], core_peer)

    def o_group_core(i):
        return send(far_rows(6, i), far_rows(7, i), oyc_send.at[i], oyc_recv.at[i], core_peer)

    def kv_chip(s):
        return send(kv_v.at[s, own_rows], kv_v.at[s, own_rows], kx_send.at[s], kx_recv.at[s], chip_peer)

    def kv_core(s):
        return send(kv_v.at[s, own_rows], kv_v.at[s, own_rows], kc_send.at[s], kc_recv.at[s], core_peer)

    def kv_chip_core(s):
        return send(kv_v.at[s, chip_rows], kv_v.at[s, chip_rows], kxc_send.at[s], kxc_recv.at[s], core_peer)

    def kv_stores(s):
        outs = ((key_hbm, 0), (value_hbm, hd))
        return [pltpu.make_async_copy(kv_v.at[s, own_rows, pl.ds(at, hd)], ref.at[s], key_sem.at[s, i]) for i, (ref, at) in enumerate(outs)]

    def kv_send(s):
        kv_chip(s).start()
        kv_core(s).start()
        start(kv_stores(s))

    x_load(0).start()
    start(wkv + own_q)

    @pl.loop(1, num_batch)
    def _(s):
        x_load(s).start()

    enter(core_peer, chip_peer, group_peer)
    start([q_chip(i) for i in range(Q_PIECES)])
    start(q_core)
    start([o_chip(i) for i in range(O_PIECES)])
    start(o_core)

    gain = gain_ref[...].astype(F32)
    block = cos_ref.shape[0]
    blocks = rows // block

    @pl.loop(0, blocks)
    def _(i):
        first = pl.ds(tp * blocks + i, 1)
        cos0, sin0 = cos0_ref[first, :], sin0_ref[first, :]
        cos_v[span(i, block), :] = cos_ref[...] * cos0 - sin_ref[...] * sin0
        sin_v[span(i, block), :] = sin_ref[...] * cos0 + cos_ref[...] * sin0

    for c in wkv + own_q:
        c.wait()

    def rope(x, cos, sin):
        a, c = x[:, :half], x[:, half:]
        return a * cos - c * sin, c * cos + a * sin

    def store_query(q, cos, sin, at, slot):
        lo, hi = rope(q, cos, sin)
        shape = q_v[at, slot, :, :half].shape
        q_v[at, slot, :, :half] = lo.astype(BF16).reshape(shape)
        q_v[at, slot, :, half:] = hi.astype(BF16).reshape(shape)

    @pl.loop(0, num_batch)
    def _(s):
        @pl.when(s == 5)
        def _():
            q_chip(0).wait_recv()
            start([q_group(0), q_chip_core(0)])

        @pl.when(s == num_batch - 1)
        def _():
            for i in range(1, Q_PIECES):
                q_chip(i).wait_recv()
                start([q_group(i), q_chip_core(i)])

        @pl.when(s > 0)
        def _():
            kv_send(s - 1)

        x_load(s).wait()
        xn = normalize(x_v[s].astype(F32), gain)
        x_v[s] = xn
        cos, sin = cos_v[...], sin_v[...]
        lo, hi = rope(dot(xn, wkv_v[0]), cos, sin)
        kv_v[s, own_rows, :half] = lo.astype(BF16)
        kv_v[s, own_rows, half:hd] = hi.astype(BF16)
        kv_v[s, own_rows, hd:] = dot(xn, wkv_v[1]).astype(BF16)
        for i in range(own_heads):
            store_query(dot(xn, w_v[i]), cos * hd**-0.5, sin * hd**-0.5, s, i)

    kv_send(num_batch - 1)

    group = 3

    @pl.loop(own_heads, heads)
    def _(slot):
        @pl.when(slot == 2)
        def _():
            wait_recv(q_core)

        @pl.when(slot == 3)
        def _():
            o_chip(0).wait_recv()
            start([o_group(0), o_chip_core(0)])

        @pl.when(slot == 5)
        def _():
            wait_recv([q_chip_core(i) for i in range(Q_PIECES)])
            o_chip(1).wait_recv()
            start([o_group(1), o_chip_core(1)])

        @pl.when(slot == 6)
        def _():
            for i in range(Q_PIECES):
                q_group(i).wait_recv()
                q_group_core(i).start()
            o_chip(2).wait_recv()
            start([o_group(2), o_chip_core(2)])

        @pl.when(slot == 7)
        def _():
            wait_recv([q_group_core(i) for i in range(Q_PIECES)])
            o_chip(3).wait_recv()
            start([o_group(3), o_chip_core(3)])

        @pl.loop(0, num_batch // group)
        def _(i):
            at = span(i, group)
            cos = jnp.concatenate([cos_v[...] * hd**-0.5] * group, axis=0)
            sin = jnp.concatenate([sin_v[...] * hd**-0.5] * group, axis=0)
            store_query(dot(x_v[at].reshape(group * rows, width), w_v[slot]), cos, sin, at, slot)

    for copies in ([q_group(i) for i in range(Q_PIECES)], [q_chip_core(i) for i in range(Q_PIECES)], [q_group_core(i) for i in range(Q_PIECES)]):
        wait_send(copies)
    for n in range(heads):
        own_o(n).start()

    @pl.loop(0, num_batch)
    def _(s):
        x_load(s).start()

    kv_chip(0).wait_recv()
    kv_chip_core(0).start()
    for i in range(O_PIECES):
        o_group(i).wait_recv()
        o_group_core(i).start()
    wait_recv(o_core + [o_chip_core(i) for i in range(O_PIECES)] + [o_group_core(i) for i in range(O_PIECES)])
    for n in range(heads):
        far_o(n).start()

    tail = 128
    col = lax.broadcasted_iota(jnp.int32, (rows, tail), 1) + (seq - tail)
    row = lax.broadcasted_iota(jnp.int32, (rows, tail), 0) + tp * rows

    def score(s, p):
        return lax.dot_general(q_v[s, p], kv_v[s, :, :hd], (((1,), (1,)), ((), ())), preferred_element_type=F32)

    def probs(sc, allowed):
        sc = jnp.concatenate([sc[:, : seq - tail], jnp.where(allowed, sc[:, seq - tail :], MASK_FILL)], axis=1)
        p = jnp.exp(sc - jnp.max(sc, axis=-1, keepdims=True))
        return (p * (1.0 / jnp.sum(p, axis=-1, keepdims=True))).astype(BF16)

    def project(s, n):
        o = jnp.concatenate([q_v[s, j] for j in range(heads)], axis=1)
        at = span(n, hd)
        x_v[s, :, at] = (x_v[s, :, at].astype(F32) + dot(o, w_v[n]).astype(BF16).astype(F32)).astype(BF16)

    gain2 = gain2_ref[...].astype(F32)

    def norm_rows(s, slot, at):
        x2_v[slot, at, :] = normalize(x_v[s, at, :].astype(F32), gain2)

    def h1_store(s):
        return pltpu.make_async_copy(x_v.at[s], h1_hbm.at[s], out_sem.at[s])

    def x2_store(s, slot):
        return pltpu.make_async_copy(x2_v.at[slot], x2_hbm.at[s], x2_sem.at[slot])

    @pl.loop(0, num_batch)
    def _(s):
        x_load(s).wait()

    for n in range(heads):
        own_o(n).wait()
        far_o(n).wait()

    last = num_batch - 1

    @pl.loop(0, num_batch)
    def _(s):
        before = lax.rem(s + last, num_batch)
        earlier = lax.rem(s + last - 1, num_batch)
        slot = lax.rem(s, 2)
        @pl.when(s < last)
        def _():
            kv_chip(s + 1).wait_recv()
            kv_chip_core(s + 1).start()

        wait_recv([kv_core(s), kv_chip_core(s)])
        allowed = (col < vlen_ref[s]) & ((col < plen_ref[s]) | (col <= row))

        @pl.when(s >= 4)
        def _():
            x2_store(s - 4, slot).wait()

        sc = score(s, 0)
        for p in range(heads):
            ahead = score(s, p + 1) if p + 1 < heads else None
            project(before, p)
            if p < 6:
                norm_rows(earlier, slot, pl.ds(p * 48, 48))
            pr = probs(sc, allowed)
            q_v[s, p] = dot(pr, kv_v[s, :, hd:]).astype(BF16)
            sc = ahead

        @pl.when(s >= 1)
        def _():
            h1_store(s - 1).start()

        @pl.when(s >= 2)
        def _():
            x2_store(s - 2, slot).start()

        @pl.when(s == 1)
        def _():
            x_load(last).start()

    x_load(last).wait()
    @pl.loop(0, heads // 2)
    def _(i):
        project(last, 2 * i)
        project(last, 2 * i + 1)

    h1_store(last).start()
    for s in (last - 1, last):
        slot = s % 2
        x2_store(s - 2, slot).wait()
        norm_rows(s, slot, slice(None))
        x2_store(s, slot).start()

    wait_send(q_core + o_core + [q_chip(i) for i in range(Q_PIECES)])
    for i in range(O_PIECES):
        wait_send([o_chip(i), o_group(i), o_chip_core(i), o_group_core(i)])

    @pl.loop(0, num_batch)
    def _(s):
        wait_send([kv_chip(s), kv_core(s), kv_chip_core(s)])
        for c in kv_stores(s):
            c.wait()
        h1_store(s).wait()

    for s in (last - 1, last):
        x2_store(s, s % 2).wait()


def attention(hidden, prefix_len, valid_len, norm_attn, norm_mlp, w_query, w_key, w_value, w_out, tp_size):
    num_batch, rows, width = hidden.shape
    hd = w_key.shape[1]
    own_heads = w_query.shape[1] // hd
    heads = own_heads * tp_size
    seq = rows * tp_size
    tables = rope_tables(seq, 16, hd)
    any_spec = pl.BlockSpec(memory_space=pl.ANY)
    smem = pl.BlockSpec(memory_space=pltpu.SMEM)
    vmem = pl.BlockSpec(memory_space=pltpu.VMEM)
    dma = pltpu.SemaphoreType.DMA
    shape = jax.ShapeDtypeStruct
    flops = 2 * num_batch * rows * (width * (2 * heads + 2) * hd + 2 * heads * hd * seq)
    out = pl.pallas_call(
        attention_kernel,
        in_specs=[smem, smem, vmem, vmem, any_spec, vmem, vmem, vmem, vmem] + [any_spec] * 4,
        out_specs=[any_spec] * 5,
        out_shape=[
            shape((num_batch, rows, width), BF16),
            shape((num_batch, rows, width), BF16),
            shape((num_batch, rows, hd), BF16),
            shape((num_batch, rows, hd), BF16),
            shape(((heads - own_heads) * hd, width), BF16),
        ],
        scratch_shapes=[
            pltpu.VMEM((num_batch, rows, width), BF16),
            pltpu.VMEM((num_batch, heads, rows, hd), BF16),
            pltpu.VMEM((num_batch, seq, 2 * hd), BF16),
            pltpu.VMEM((heads, width, hd), BF16),
            pltpu.VMEM((2, width, hd), BF16),
            pltpu.VMEM((rows, hd // 2), F32),
            pltpu.VMEM((rows, hd // 2), F32),
            pltpu.VMEM((2, rows, width), BF16),
            dma((num_batch,)),
            dma((2,)),
            dma((heads, 2)),
            dma((num_batch,)),
            dma((2,)),
            dma((num_batch, 2)),
        ]
        + [dma((own_heads,))] * 2
        + [dma((Q_PIECES,))] * 8
        + [dma((1,))] * 2
        + [dma((O_PIECES,))] * 8
        + [dma((num_batch,))] * 6,
        compiler_params=pltpu.CompilerParams(vmem_limit_bytes=VMEM_LIMIT, collective_id=1, has_side_effects=True),
        cost_estimate=pl.CostEstimate(flops=flops, bytes_accessed=num_batch * rows * width * 6, transcendentals=num_batch * rows * heads * seq),
        name="attention",
    )(prefix_len, valid_len, norm_attn, norm_mlp, hidden, *(jnp.asarray(t) for t in tables), w_query, w_key, w_value, w_out)
    return out[:4]


GELU_LINEAR = 0.7978845608028654
GELU_CUBIC = GELU_LINEAR * 0.044715


def expand(x_ref, wg_ref, wu_ref, act_ref):
    block = 256
    for n in range(0, act_ref.shape[1], block):
        at = slice(n, n + block)
        gate = dot(x_ref[...], wg_ref[:, at])
        up = dot(x_ref[...], wu_ref[:, at])
        t = jnp.tanh(gate * (GELU_CUBIC * (gate * gate) + GELU_LINEAR))
        act_ref[:, at] = ((0.5 * gate) * up * (1.0 + t)).astype(BF16)


def mlp_kernel(x_hbm, wg_hbm, wu_hbm, wd_hbm, out_hbm, pg_hbm, pu_hbm, pd_hbm, rg_hbm, ru_hbm, rd_hbm,
               x_v, acc_v, act_v, wg_v, wu_v, wd_v, load_sem, x_sem, out_sem,
               p_send, p_recv, a_send, a_recv, ac_send, ac_recv, b_send, b_recv, bc_send, bc_recv):
    rows, width = x_v.shape
    tile = act_v.shape[1]
    tiles = rows // tile
    unit = wg_v.shape[2]
    piece = unit // 2
    own = wg_hbm.shape[1] // unit
    pieces = own // 2 * 2
    groups, per_group = rg_hbm.shape[:2]
    steps = 2 * own + groups * per_group - LAST_UNITS
    dp, tp, chip_tp, core_peer, chip_peer, group_peer = peers()

    def piece_refs(group, j):
        at = pl.ds(pl.multiple_of(lax.rem(j, 2) * piece, piece), piece)
        return rg_hbm.at[group, j // 2, :, at], ru_hbm.at[group, j // 2, :, at], rd_hbm.at[group, j // 2, at, :]

    def own_copies():
        refs = ((wg_hbm, pg_hbm), (wu_hbm, pu_hbm), (wd_hbm, pd_hbm))
        return [send(src, dst, p_send.at[i], p_recv.at[i], core_peer) for i, (src, dst) in enumerate(refs)]

    def chip_copies(j):
        at = pl.ds(pl.multiple_of(dp * pieces * piece + j * piece, piece), piece)
        src = (wg_hbm.at[:, at], wu_hbm.at[:, at], wd_hbm.at[at, :])
        return [send(s, d, a_send.at[j, i], a_recv.at[j, i], chip_peer) for i, (s, d) in enumerate(zip(src, piece_refs(0, j)))]

    def relay(j, source, target, send_sems, recv_sems, peer):
        pairs = zip(piece_refs(source, j), piece_refs(target, j))
        return [send(s, d, send_sems.at[j, i], recv_sems.at[j, i], peer) for i, (s, d) in enumerate(pairs)]

    def core_a(j):
        return relay(j, 0, 1, ac_send, ac_recv, core_peer)

    def group_a(j):
        return relay(j, 0, 2, b_send, b_recv, group_peer)

    def core_b(j):
        return relay(j, 2, 3, bc_send, bc_recv, core_peer)

    def x_copy(m):
        at = span(m, tile)
        return pltpu.make_async_copy(x_hbm.at[at], x_v.at[at], x_sem.at[m])

    def load(src, slot):
        return [pltpu.make_async_copy(s, d.at[slot], load_sem.at[slot, i]) for i, (s, d) in enumerate(zip(src, (wg_v, wu_v, wd_v)))]

    def own_load(u, slot):
        at = pl.ds(pl.multiple_of(u * unit, unit), unit)
        return load((wg_hbm.at[:, at], wu_hbm.at[:, at], wd_hbm.at[at, :]), slot)

    def peer_load(u, slot):
        at = pl.ds(pl.multiple_of((u - own) * unit, unit), unit)
        return load((pg_hbm.at[:, at], pu_hbm.at[:, at], pd_hbm.at[at, :]), slot)

    def far_load(u, slot):
        i = u - 2 * own
        g = lax.rem(i, groups)
        p = i // groups
        return load((rg_hbm.at[g, p], ru_hbm.at[g, p], rd_hbm.at[g, p]), slot)

    x_copy(0).start()
    start(own_load(0, 0))
    enter(core_peer, chip_peer, group_peer)
    start(own_copies())

    @pl.loop(0, pieces)
    def _(j):
        start(chip_copies(j))

    @pl.loop(0, rows // 96)
    def _(i):
        acc_v[span(i, 96), :] = jnp.zeros((96, width), F32)

    def out_copy(m):
        at = span(m, tile)
        return pltpu.make_async_copy(x_v.at[at], out_hbm.at[at], out_sem.at[m])

    first_a, first_b, every = 4, 8, 3

    @pl.loop(0, steps)
    def _(s):
        slot = lax.rem(s, 2)

        @pl.when((s >= first_a) & (s < first_a + every * pieces) & (lax.rem(s - first_a + every, every) == 0))
        def _():
            j = (s - first_a) // every
            wait_recv(chip_copies(j))
            start(group_a(j))
            start(core_a(j))

        @pl.when((s >= first_b) & (s < first_b + every * pieces) & (lax.rem(s - first_b + 2 * every, every) == 0))
        def _():
            j = (s - first_b) // every
            wait_recv(group_a(j))
            start(core_b(j))

        u = s + 1

        @pl.when(u < own)
        def _():
            start(own_load(u, 1 - slot))

        @pl.when(u == own)
        def _():
            wait_recv(own_copies())

        @pl.when((u >= own) & (u < 2 * own))
        def _():
            start(peer_load(u, 1 - slot))

        @pl.when((u >= 2 * own) & (u < steps))
        def _():
            g = lax.rem(u - 2 * own, groups)
            p = (u - 2 * own) // groups

            @pl.when(g == 1)
            def _():
                for j in (2 * p, 2 * p + 1):
                    wait_recv(core_a(j))

            @pl.when(g == 3)
            def _():
                for j in (2 * p, 2 * p + 1):
                    wait_recv(core_b(j))

            start(far_load(u, 1 - slot))

        for c in own_load(0, slot):
            c.wait()

        def compute(m, at, act):
            expand(x_v.at[at], wg_v.at[slot], wu_v.at[slot], act)
            for n in range(0, width, unit):
                acc_v[at, n : n + unit] += dot(act[...], wd_v[slot, :, n : n + unit])

        @pl.when((s == 0) | (s == steps - 1))
        def _():
            @pl.when(s == 0)
            def _():
                x_copy(0).wait()
                for m in range(1, tiles):
                    x_copy(m).start()

            @pl.loop(0, tiles)
            def _(m):
                @pl.when((s == 0) & (m > 0))
                def _():
                    x_copy(m).wait()

                compute(m, span(m, tile), act_v.at[0])

                @pl.when(s == steps - 1)
                def _():
                    @pl.loop(0, tile // 96)
                    def _(i):
                        at = span(m * (tile // 96) + i, 96)
                        x_v[at, :] = acc_v[at, :].astype(BF16)

                    out_copy(m).start()

        @pl.when((s > 0) & (s < steps - 1))
        def _():
            for m in range(tiles):
                compute(m, pl.ds(m * tile, tile), act_v.at[m % 2])

    for j in (pieces - 2, pieces - 1):
        wait_recv(core_b(j))
    wait_send(own_copies())

    @pl.loop(0, pieces)
    def _(j):
        for copies in (chip_copies(j), group_a(j), core_a(j), core_b(j)):
            wait_send(copies)

    for m in range(tiles):
        out_copy(m).wait()


def mlp(x2, w_gate, w_up, w_down):
    rows, width = x2.shape
    ff = w_gate.shape[1]
    unit = 512
    tile = rows // 6
    far = ff // 2 // unit
    pieces = 2 * far
    shapes = [(rows, width), (width, ff), (width, ff), (ff, width), (4, far, width, unit), (4, far, width, unit), (4, far, unit, width)]
    any_spec = pl.BlockSpec(memory_space=pl.ANY)
    dma = pltpu.SemaphoreType.DMA
    out = pl.pallas_call(
        mlp_kernel,
        in_specs=[any_spec] * 4,
        out_specs=[any_spec] * 7,
        out_shape=[jax.ShapeDtypeStruct(s, BF16) for s in shapes],
        scratch_shapes=[
            pltpu.VMEM((rows, width), BF16),
            pltpu.VMEM((rows, width), F32),
            pltpu.VMEM((2, tile, unit), BF16),
            pltpu.VMEM((2, width, unit), BF16),
            pltpu.VMEM((2, width, unit), BF16),
            pltpu.VMEM((2, unit, width), BF16),
            dma((2, 3)),
            dma((rows // tile,)),
            dma((rows // tile,)),
            dma((3,)),
            dma((3,)),
        ]
        + [dma((pieces, 3))] * 8,
        compiler_params=pltpu.CompilerParams(vmem_limit_bytes=VMEM_LIMIT, collective_id=0, has_side_effects=True),
        cost_estimate=pl.CostEstimate(flops=2 * rows * width * ff * 3 * 4, bytes_accessed=4 * 3 * width * ff * 2, transcendentals=0),
        name="mlp",
    )(x2, w_gate, w_up, w_down)
    return out[0], out[4:]


def last_kernel(x_ref, part_ref, h_ref, wg_ref, wu_ref, wd_ref, key_hbm, value_hbm, out_ref, key_out, value_out, act_v, cache_v, sem):
    i = pl.program_id(0)
    pairs = ((key_hbm, key_out), (value_hbm, value_out))
    loads = [pltpu.make_async_copy(src, cache_v.at[n], sem.at[n]) for n, (src, _) in enumerate(pairs)]
    stores = [pltpu.make_async_copy(cache_v.at[n], dst, sem.at[n]) for n, (_, dst) in enumerate(pairs)]

    @pl.when(i == 0)
    def _():
        start(loads)

    @pl.when(i == 1)
    def _():
        for load, store in zip(loads, stores):
            load.wait()
            store.start()

    expand(x_ref, wg_ref.at[0, 0], wu_ref.at[0, 0], act_v)
    block = 512
    for n in range(0, out_ref.shape[1], block):
        at = slice(n, n + block)
        total = part_ref[:, at].astype(F32) + dot(act_v[...], wd_ref[0, 0, :, at])
        out_ref[:, at] = (h_ref[:, at].astype(F32) + total.astype(BF16).astype(F32)).astype(BF16)

    @pl.when(i == pl.num_programs(0) - 1)
    def _():
        for store in stores:
            store.wait()


def finish(x2, part, h1, far_weights, key, value):
    rows, width = x2.shape
    tile = rows // 6
    groups, per_group = far_weights[0].shape[:2]
    row_block = pl.BlockSpec((tile, width), lambda i: (i, 0))
    any_spec = pl.BlockSpec(memory_space=pl.ANY)

    def weight_block(w):
        return pl.BlockSpec((1, 1) + w.shape[2:], lambda i: (groups - 1, per_group - 1, 0, 0), pipeline_mode=pl.Buffered(1))

    unit = far_weights[0].shape[3]
    shape = jax.ShapeDtypeStruct
    return pl.pallas_call(
        last_kernel,
        grid=(rows // tile,),
        in_specs=[row_block] * 3 + [weight_block(w) for w in far_weights] + [any_spec] * 2,
        out_specs=[row_block, any_spec, any_spec],
        out_shape=[shape(x2.shape, BF16), shape(key.shape, BF16), shape(value.shape, BF16)],
        scratch_shapes=[pltpu.VMEM((tile, unit), BF16), pltpu.VMEM((2,) + key.shape, BF16), pltpu.SemaphoreType.DMA((2,))],
        compiler_params=pltpu.CompilerParams(dimension_semantics=("arbitrary",), vmem_limit_bytes=60 << 20),
        cost_estimate=pl.CostEstimate(flops=6 * rows * width * unit, bytes_accessed=8 * rows * width, transcendentals=0),
        name="finish",
    )(x2, part, h1, *far_weights, key, value)


def solution(mesh):
    tp_size = mesh.shape["tp"]
    row_spec = P("dp", "tp", None)
    arg_specs = (row_spec, P("dp"), P("dp"), P(), P(None, "tp"), P(), P(), P("tp", None), P(), P(None, "tp"), P(None, "tp"), P("tp", None))

    def local_layer(hidden, prefix_len, valid_len, norm_attn, w_query, w_key, w_value, w_out, norm_mlp, w_gate, w_up, w_down):
        h1, x2, key, value = attention(hidden, prefix_len, valid_len, norm_attn, norm_mlp, w_query, w_key, w_value, w_out, tp_size)
        flat = (-1, hidden.shape[-1])
        x2 = x2.reshape(flat)
        part, far_weights = mlp(x2, w_gate, w_up, w_down)
        out, key, value = finish(x2, part, h1.reshape(flat), far_weights, key, value)
        return out.reshape(hidden.shape), key, value

    return jax.shard_map(local_layer, mesh=mesh, in_specs=arg_specs, out_specs=(row_spec, row_spec, row_spec), check_vma=False)
```

```python
import functools

import jax
import jax.numpy as jnp
import numpy as np
from jax import lax
from jax.experimental import pallas as pl
from jax.experimental.pallas import tpu as pltpu
from jax.sharding import PartitionSpec as P

NORM_EPS = 1e-6
ROPE_BASE = 10000.0
MASK_FILL = -1e30
F32 = jnp.float32
BF16 = jnp.bfloat16
MESH = pl.DeviceIdType.MESH
VMEM_LIMIT = 67043328


def rope_tables(seq, block, head_dim):
    inv_freq = ROPE_BASE ** (-2.0 * np.arange(head_dim // 2) / head_dim)
    angles = np.arange(block)[:, None] * inv_freq[None, :]
    starts = np.arange(0, seq, block)[:, None] * inv_freq[None, :]
    return tuple(f(a).astype(np.float32) for a in (angles, starts) for f in (np.cos, np.sin))


def normalize(rows, gain):
    inv = lax.rsqrt(jnp.mean(rows * rows, axis=-1, keepdims=True) + NORM_EPS)
    return (rows * inv * (1.0 + gain)).astype(BF16)


def dot(a, b):
    return jnp.dot(a, b, preferred_element_type=F32)


def span(index, size):
    return pl.ds(pl.multiple_of(index * size, size), size)


def start(copies):
    for c in copies:
        c.start()


def wait_recv(copies):
    for c in copies:
        c.wait_recv()


def wait_send(copies):
    for c in copies:
        c.wait_send()


def send(src, dst, send_sem, recv_sem, peer):
    return pltpu.make_async_remote_copy(src_ref=src, dst_ref=dst, send_sem=send_sem, recv_sem=recv_sem, device_id=peer, device_id_type=MESH)


def peers():
    dp = lax.axis_index("dp")
    tp = lax.axis_index("tp")
    core_tp = tp + 1 - 2 * lax.rem(tp, 2)
    chip_tp = lax.rem(tp + 2, 4)
    return dp, tp, chip_tp, {"tp": core_tp}, {"tp": chip_tp}, {"dp": 1 - dp}


def enter(*others):
    barrier = pltpu.get_barrier_semaphore()
    for peer in others:
        pl.semaphore_signal(barrier, inc=1, device_id=peer, device_id_type=MESH)
    pl.semaphore_wait(barrier, len(others))


Q_PIECES = 2
O_PIECES = 4
LAST_UNITS = 1


def attention_kernel(plen_ref, vlen_ref, gain_ref, gain2_ref, h_hbm, cos_ref, sin_ref, cos0_ref, sin0_ref, wq_hbm, wk_hbm, wv_hbm, wo_hbm,
                     h1_hbm, x2_hbm, key_hbm, value_hbm, wo_far,
                     x_v, q_v, kv_v, w_v, wkv_v, cos_v, sin_v, x2_v,
                     x_sem, wkv_sem, w_sem, out_sem, x2_sem, key_sem,
                     qc_send, qc_recv, qx_send, qx_recv, qy_send, qy_recv, qxc_send, qxc_recv, qyc_send, qyc_recv,
                     oc_send, oc_recv, ox_send, ox_recv, oy_send, oy_recv, oxc_send, oxc_recv, oyc_send, oyc_recv,
                     kx_send, kx_recv, kc_send, kc_recv, kxc_send, kxc_recv):
    num_batch, rows, width = x_v.shape
    heads, hd = q_v.shape[1], q_v.shape[3]
    seq = kv_v.shape[1]
    own_heads = wq_hbm.shape[1] // hd
    half = hd // 2
    dp, tp, chip_tp, core_peer, chip_peer, group_peer = peers()
    own_rows = span(tp, rows)
    chip_rows = span(chip_tp, rows)

    wkv = [pltpu.make_async_copy(w, wkv_v.at[i], wkv_sem.at[i]) for i, w in enumerate((wk_hbm, wv_hbm))]
    own_q = [pltpu.make_async_copy(wq_hbm.at[:, pl.ds(i * hd, hd)], w_v.at[i], w_sem.at[i, 0]) for i in range(own_heads)]

    def x_load(s):
        return pltpu.make_async_copy(h_hbm.at[s], x_v.at[s], x_sem.at[s])

    def own_o(n):
        return pltpu.make_async_copy(wo_hbm.at[:, pl.ds(n * hd, hd)], w_v.at[n, pl.ds(0, own_heads * hd)], w_sem.at[n, 0])

    def far_o(n):
        size = (heads - own_heads) * hd
        return pltpu.make_async_copy(wo_far.at[:, pl.ds(n * hd, hd)], w_v.at[n, pl.ds(own_heads * hd, size)], w_sem.at[n, 1])

    q_core = [send(wq_hbm.at[:, pl.ds(i * hd, hd)], w_v.at[own_heads + i], qc_send.at[i], qc_recv.at[i], core_peer) for i in range(own_heads)]
    q_rows = width // Q_PIECES

    def q_chip(i):
        return send(wq_hbm.at[pl.ds(i * q_rows, q_rows), span(dp, hd)], w_v.at[4, pl.ds(i * q_rows, q_rows)], qx_send.at[i], qx_recv.at[i], chip_peer)

    def q_move(src, dst, i, send_sem, recv_sem, peer):
        at = pl.ds(i * q_rows, q_rows)
        return send(w_v.at[src, at], w_v.at[dst, at], send_sem.at[i], recv_sem.at[i], peer)

    def q_group(i):
        return q_move(4, 6, i, qy_send, qy_recv, group_peer)

    def q_chip_core(i):
        return q_move(4, 5, i, qxc_send, qxc_recv, core_peer)

    def q_group_core(i):
        return q_move(6, 7, i, qyc_send, qyc_recv, core_peer)

    own_width = own_heads * hd
    o_rows = hd // O_PIECES
    o_core = [send(wo_hbm, wo_far.at[pl.ds(0, own_width)], oc_send.at[0], oc_recv.at[0], core_peer)]

    def far_rows(slot, i):
        return wo_far.at[pl.ds((slot - own_heads) * hd + i * o_rows, o_rows)]

    def o_chip(i):
        src = wo_hbm.at[pl.ds(pl.multiple_of(dp * hd + i * o_rows, o_rows), o_rows)]
        return send(src, far_rows(4, i), ox_send.at[i], ox_recv.at[i], chip_peer)

    def o_group(i):
        return send(far_rows(4, i), far_rows(6, i), oy_send.at[i], oy_recv.at[i], group_peer)

    def o_chip_core(i):
        return send(far_rows(4, i), far_rows(5, i), oxc_send.at[i], oxc_recv.at[i], core_peer)

    def o_group_core(i):
        return send(far_rows(6, i), far_rows(7, i), oyc_send.at[i], oyc_recv.at[i], core_peer)

    def kv_chip(s):
        return send(kv_v.at[s, own_rows], kv_v.at[s, own_rows], kx_send.at[s], kx_recv.at[s], chip_peer)

    def kv_core(s):
        return send(kv_v.at[s, own_rows], kv_v.at[s, own_rows], kc_send.at[s], kc_recv.at[s], core_peer)

    def kv_chip_core(s):
        return send(kv_v.at[s, chip_rows], kv_v.at[s, chip_rows], kxc_send.at[s], kxc_recv.at[s], core_peer)

    def kv_stores(s):
        outs = ((key_hbm, 0), (value_hbm, hd))
        return [pltpu.make_async_copy(kv_v.at[s, own_rows, pl.ds(at, hd)], ref.at[s], key_sem.at[s, i]) for i, (ref, at) in enumerate(outs)]

    def kv_send(s):
        kv_chip(s).start()
        kv_core(s).start()
        start(kv_stores(s))

    x_load(0).start()
    start(wkv + own_q)

    @pl.loop(1, num_batch)
    def _(s):
        x_load(s).start()

    enter(core_peer, chip_peer, group_peer)
    start([q_chip(i) for i in range(Q_PIECES)])
    start(q_core)
    start([o_chip(i) for i in range(O_PIECES)])
    start(o_core)

    gain = gain_ref[...].astype(F32)
    block = cos_ref.shape[0]
    blocks = rows // block

    @pl.loop(0, blocks)
    def _(i):
        first = pl.ds(tp * blocks + i, 1)
        cos0, sin0 = cos0_ref[first, :], sin0_ref[first, :]
        cos_v[span(i, block), :] = cos_ref[...] * cos0 - sin_ref[...] * sin0
        sin_v[span(i, block), :] = sin_ref[...] * cos0 + cos_ref[...] * sin0

    for c in wkv + own_q:
        c.wait()

    def rope(x, cos, sin):
        a, c = x[:, :half], x[:, half:]
        return a * cos - c * sin, c * cos + a * sin

    def store_query(q, cos, sin, at, slot):
        lo, hi = rope(q, cos, sin)
        shape = q_v[at, slot, :, :half].shape
        q_v[at, slot, :, :half] = lo.astype(BF16).reshape(shape)
        q_v[at, slot, :, half:] = hi.astype(BF16).reshape(shape)

    @pl.loop(0, num_batch)
    def _(s):
        @pl.when(s == 5)
        def _():
            q_chip(0).wait_recv()
            start([q_group(0), q_chip_core(0)])

        @pl.when(s == num_batch - 1)
        def _():
            for i in range(1, Q_PIECES):
                q_chip(i).wait_recv()
                start([q_group(i), q_chip_core(i)])

        @pl.when(s > 0)
        def _():
            kv_send(s - 1)

        x_load(s).wait()
        xn = normalize(x_v[s].astype(F32), gain)
        x_v[s] = xn
        cos, sin = cos_v[...], sin_v[...]
        lo, hi = rope(dot(xn, wkv_v[0]), cos, sin)
        kv_v[s, own_rows, :half] = lo.astype(BF16)
        kv_v[s, own_rows, half:hd] = hi.astype(BF16)
        kv_v[s, own_rows, hd:] = dot(xn, wkv_v[1]).astype(BF16)
        for i in range(own_heads):
            store_query(dot(xn, w_v[i]), cos * hd**-0.5, sin * hd**-0.5, s, i)

    kv_send(num_batch - 1)

    group = 3

    @pl.loop(own_heads, heads)
    def _(slot):
        @pl.when(slot == 2)
        def _():
            wait_recv(q_core)

        @pl.when(slot == 3)
        def _():
            o_chip(0).wait_recv()
            start([o_group(0), o_chip_core(0)])

        @pl.when(slot == 5)
        def _():
            wait_recv([q_chip_core(i) for i in range(Q_PIECES)])
            o_chip(1).wait_recv()
            start([o_group(1), o_chip_core(1)])

        @pl.when(slot == 6)
        def _():
            for i in range(Q_PIECES):
                q_group(i).wait_recv()
                q_group_core(i).start()
            o_chip(2).wait_recv()
            start([o_group(2), o_chip_core(2)])

        @pl.when(slot == 7)
        def _():
            wait_recv([q_group_core(i) for i in range(Q_PIECES)])
            o_chip(3).wait_recv()
            start([o_group(3), o_chip_core(3)])

        @pl.loop(0, num_batch // group)
        def _(i):
            at = span(i, group)
            cos = jnp.concatenate([cos_v[...] * hd**-0.5] * group, axis=0)
            sin = jnp.concatenate([sin_v[...] * hd**-0.5] * group, axis=0)
            store_query(dot(x_v[at].reshape(group * rows, width), w_v[slot]), cos, sin, at, slot)

    for copies in ([q_group(i) for i in range(Q_PIECES)], [q_chip_core(i) for i in range(Q_PIECES)], [q_group_core(i) for i in range(Q_PIECES)]):
        wait_send(copies)
    for n in range(heads):
        own_o(n).start()

    @pl.loop(0, num_batch)
    def _(s):
        x_load(s).start()

    kv_chip(0).wait_recv()
    kv_chip_core(0).start()
    for i in range(O_PIECES):
        o_group(i).wait_recv()
        o_group_core(i).start()
    wait_recv(o_core + [o_chip_core(i) for i in range(O_PIECES)] + [o_group_core(i) for i in range(O_PIECES)])
    for n in range(heads):
        far_o(n).start()

    tail = 128
    col = lax.broadcasted_iota(jnp.int32, (rows, tail), 1) + (seq - tail)
    row = lax.broadcasted_iota(jnp.int32, (rows, tail), 0) + tp * rows

    def score(s, p):
        return lax.dot_general(q_v[s, p], kv_v[s, :, :hd], (((1,), (1,)), ((), ())), preferred_element_type=F32)

    def probs(sc, allowed):
        sc = jnp.concatenate([sc[:, : seq - tail], jnp.where(allowed, sc[:, seq - tail :], MASK_FILL)], axis=1)
        p = jnp.exp(sc - jnp.max(sc, axis=-1, keepdims=True))
        return (p * (1.0 / jnp.sum(p, axis=-1, keepdims=True))).astype(BF16)

    def project(s, n):
        o = jnp.concatenate([q_v[s, j] for j in range(heads)], axis=1)
        at = span(n, hd)
        x_v[s, :, at] = (x_v[s, :, at].astype(F32) + dot(o, w_v[n]).astype(BF16).astype(F32)).astype(BF16)

    gain2 = gain2_ref[...].astype(F32)

    def norm_rows(s, slot, at):
        x2_v[slot, at, :] = normalize(x_v[s, at, :].astype(F32), gain2)

    def h1_store(s):
        return pltpu.make_async_copy(x_v.at[s], h1_hbm.at[s], out_sem.at[s])

    def x2_store(s, slot):
        return pltpu.make_async_copy(x2_v.at[slot], x2_hbm.at[s], x2_sem.at[slot])

    @pl.loop(0, num_batch)
    def _(s):
        x_load(s).wait()

    for n in range(heads):
        own_o(n).wait()
        far_o(n).wait()

    last = num_batch - 1

    @pl.loop(0, num_batch)
    def _(s):
        before = lax.rem(s + last, num_batch)
        earlier = lax.rem(s + last - 1, num_batch)
        slot = lax.rem(s, 2)
        @pl.when(s < last)
        def _():
            kv_chip(s + 1).wait_recv()
            kv_chip_core(s + 1).start()

        wait_recv([kv_core(s), kv_chip_core(s)])
        allowed = (col < vlen_ref[s]) & ((col < plen_ref[s]) | (col <= row))

        @pl.when(s >= 4)
        def _():
            x2_store(s - 4, slot).wait()

        sc = score(s, 0)
        for p in range(heads):
            ahead = score(s, p + 1) if p + 1 < heads else None
            project(before, p)
            if p < 6:
                norm_rows(earlier, slot, pl.ds(p * 48, 48))
            pr = probs(sc, allowed)
            q_v[s, p] = dot(pr, kv_v[s, :, hd:]).astype(BF16)
            sc = ahead

        @pl.when(s >= 1)
        def _():
            h1_store(s - 1).start()

        @pl.when(s >= 2)
        def _():
            x2_store(s - 2, slot).start()

        @pl.when(s == 1)
        def _():
            x_load(last).start()

    x_load(last).wait()
    @pl.loop(0, heads // 2)
    def _(i):
        project(last, 2 * i)
        project(last, 2 * i + 1)

    h1_store(last).start()
    for s in (last - 1, last):
        slot = s % 2
        x2_store(s - 2, slot).wait()
        norm_rows(s, slot, slice(None))
        x2_store(s, slot).start()

    wait_send(q_core + o_core + [q_chip(i) for i in range(Q_PIECES)])
    for i in range(O_PIECES):
        wait_send([o_chip(i), o_group(i), o_chip_core(i), o_group_core(i)])

    @pl.loop(0, num_batch)
    def _(s):
        wait_send([kv_chip(s), kv_core(s), kv_chip_core(s)])
        for c in kv_stores(s):
            c.wait()
        h1_store(s).wait()

    for s in (last - 1, last):
        x2_store(s, s % 2).wait()


def attention(hidden, prefix_len, valid_len, norm_attn, norm_mlp, w_query, w_key, w_value, w_out, tp_size):
    num_batch, rows, width = hidden.shape
    hd = w_key.shape[1]
    own_heads = w_query.shape[1] // hd
    heads = own_heads * tp_size
    seq = rows * tp_size
    tables = rope_tables(seq, 16, hd)
    any_spec = pl.BlockSpec(memory_space=pl.ANY)
    smem = pl.BlockSpec(memory_space=pltpu.SMEM)
    vmem = pl.BlockSpec(memory_space=pltpu.VMEM)
    dma = pltpu.SemaphoreType.DMA
    shape = jax.ShapeDtypeStruct
    flops = 2 * num_batch * rows * (width * (2 * heads + 2) * hd + 2 * heads * hd * seq)
    out = pl.pallas_call(
        attention_kernel,
        in_specs=[smem, smem, vmem, vmem, any_spec, vmem, vmem, vmem, vmem] + [any_spec] * 4,
        out_specs=[any_spec] * 5,
        out_shape=[
            shape((num_batch, rows, width), BF16),
            shape((num_batch, rows, width), BF16),
            shape((num_batch, rows, hd), BF16),
            shape((num_batch, rows, hd), BF16),
            shape(((heads - own_heads) * hd, width), BF16),
        ],
        scratch_shapes=[
            pltpu.VMEM((num_batch, rows, width), BF16),
            pltpu.VMEM((num_batch, heads, rows, hd), BF16),
            pltpu.VMEM((num_batch, seq, 2 * hd), BF16),
            pltpu.VMEM((heads, width, hd), BF16),
            pltpu.VMEM((2, width, hd), BF16),
            pltpu.VMEM((rows, hd // 2), F32),
            pltpu.VMEM((rows, hd // 2), F32),
            pltpu.VMEM((2, rows, width), BF16),
            dma((num_batch,)),
            dma((2,)),
            dma((heads, 2)),
            dma((num_batch,)),
            dma((2,)),
            dma((num_batch, 2)),
        ]
        + [dma((own_heads,))] * 2
        + [dma((Q_PIECES,))] * 8
        + [dma((1,))] * 2
        + [dma((O_PIECES,))] * 8
        + [dma((num_batch,))] * 6,
        compiler_params=pltpu.CompilerParams(vmem_limit_bytes=VMEM_LIMIT, collective_id=1, has_side_effects=True),
        cost_estimate=pl.CostEstimate(flops=flops, bytes_accessed=num_batch * rows * width * 6, transcendentals=num_batch * rows * heads * seq),
        name="attention",
    )(prefix_len, valid_len, norm_attn, norm_mlp, hidden, *(jnp.asarray(t) for t in tables), w_query, w_key, w_value, w_out)
    return out[:4]


GELU_LINEAR = 0.7978845608028654
GELU_CUBIC = GELU_LINEAR * 0.044715


def expand(x_ref, wg_ref, wu_ref, act_ref):
    block = 256
    for n in range(0, act_ref.shape[1], block):
        at = slice(n, n + block)
        gate = dot(x_ref[...], wg_ref[:, at])
        up = dot(x_ref[...], wu_ref[:, at])
        t = jnp.tanh(gate * (GELU_CUBIC * (gate * gate) + GELU_LINEAR))
        act_ref[:, at] = ((0.5 * gate) * up * (1.0 + t)).astype(BF16)


def mlp_kernel(x_hbm, wg_hbm, wu_hbm, wd_hbm, out_hbm, pg_hbm, pu_hbm, pd_hbm, rg_hbm, ru_hbm, rd_hbm,
               x_v, acc_v, act_v, wg_v, wu_v, wd_v, load_sem, x_sem, out_sem,
               p_send, p_recv, a_send, a_recv, ac_send, ac_recv, b_send, b_recv, bc_send, bc_recv):
    rows, width = x_v.shape
    tile = act_v.shape[1]
    tiles = rows // tile
    unit = wg_v.shape[2]
    piece = unit // 2
    own = wg_hbm.shape[1] // unit
    pieces = own // 2 * 2
    groups, per_group = rg_hbm.shape[:2]
    steps = 2 * own + groups * per_group - LAST_UNITS
    dp, tp, chip_tp, core_peer, chip_peer, group_peer = peers()

    def piece_refs(group, j):
        at = pl.ds(pl.multiple_of(lax.rem(j, 2) * piece, piece), piece)
        return rg_hbm.at[group, j // 2, :, at], ru_hbm.at[group, j // 2, :, at], rd_hbm.at[group, j // 2, at, :]

    def own_copies():
        refs = ((wg_hbm, pg_hbm), (wu_hbm, pu_hbm), (wd_hbm, pd_hbm))
        return [send(src, dst, p_send.at[i], p_recv.at[i], core_peer) for i, (src, dst) in enumerate(refs)]

    def chip_copies(j):
        at = pl.ds(pl.multiple_of(dp * pieces * piece + j * piece, piece), piece)
        src = (wg_hbm.at[:, at], wu_hbm.at[:, at], wd_hbm.at[at, :])
        return [send(s, d, a_send.at[j, i], a_recv.at[j, i], chip_peer) for i, (s, d) in enumerate(zip(src, piece_refs(0, j)))]

    def relay(j, source, target, send_sems, recv_sems, peer):
        pairs = zip(piece_refs(source, j), piece_refs(target, j))
        return [send(s, d, send_sems.at[j, i], recv_sems.at[j, i], peer) for i, (s, d) in enumerate(pairs)]

    def core_a(j):
        return relay(j, 0, 1, ac_send, ac_recv, core_peer)

    def group_a(j):
        return relay(j, 0, 2, b_send, b_recv, group_peer)

    def core_b(j):
        return relay(j, 2, 3, bc_send, bc_recv, core_peer)

    def x_copy(m):
        at = span(m, tile)
        return pltpu.make_async_copy(x_hbm.at[at], x_v.at[at], x_sem.at[m])

    def load(src, slot):
        return [pltpu.make_async_copy(s, d.at[slot], load_sem.at[slot, i]) for i, (s, d) in enumerate(zip(src, (wg_v, wu_v, wd_v)))]

    def own_load(u, slot):
        at = pl.ds(pl.multiple_of(u * unit, unit), unit)
        return load((wg_hbm.at[:, at], wu_hbm.at[:, at], wd_hbm.at[at, :]), slot)

    def peer_load(u, slot):
        at = pl.ds(pl.multiple_of((u - own) * unit, unit), unit)
        return load((pg_hbm.at[:, at], pu_hbm.at[:, at], pd_hbm.at[at, :]), slot)

    def far_load(u, slot):
        i = u - 2 * own
        g = lax.rem(i, groups)
        p = i // groups
        return load((rg_hbm.at[g, p], ru_hbm.at[g, p], rd_hbm.at[g, p]), slot)

    x_copy(0).start()
    start(own_load(0, 0))
    enter(core_peer, chip_peer, group_peer)
    start(own_copies())

    @pl.loop(0, pieces)
    def _(j):
        start(chip_copies(j))

    @pl.loop(0, rows // 96)
    def _(i):
        acc_v[span(i, 96), :] = jnp.zeros((96, width), F32)

    def out_copy(m):
        at = span(m, tile)
        return pltpu.make_async_copy(x_v.at[at], out_hbm.at[at], out_sem.at[m])

    @pl.loop(0, steps)
    def _(s):
        slot = lax.rem(s, 2)

        turn = (s - 3) // 3
        both = ((s >= 7) & (s <= 16) & (lax.rem(s, 3) == 1)) | ((s >= 20) & (s <= 26) & (lax.rem(s, 3) == 2))

        @pl.when((s == 3) | both)
        def _():
            wait_recv(chip_copies(turn))
            start(group_a(turn))
            start(core_a(turn))

        @pl.when(both | (s == 29))
        def _():
            wait_recv(group_a(turn - 1))
            start(core_b(turn - 1))

        u = s + 1

        @pl.when(u < own)
        def _():
            start(own_load(u, 1 - slot))

        @pl.when(u == own)
        def _():
            wait_recv(own_copies())

        @pl.when((u >= own) & (u < 2 * own))
        def _():
            start(peer_load(u, 1 - slot))

        @pl.when((u >= 2 * own) & (u < steps))
        def _():
            g = lax.rem(u - 2 * own, groups)
            p = (u - 2 * own) // groups

            @pl.when(g == 1)
            def _():
                for j in (2 * p, 2 * p + 1):
                    wait_recv(core_a(j))

            @pl.when(g == 3)
            def _():
                for j in (2 * p, 2 * p + 1):
                    wait_recv(core_b(j))

            start(far_load(u, 1 - slot))

        for c in own_load(0, slot):
            c.wait()

        def compute(m, at, act):
            expand(x_v.at[at], wg_v.at[slot], wu_v.at[slot], act)
            for n in range(0, width, unit):
                acc_v[at, n : n + unit] += dot(act[...], wd_v[slot, :, n : n + unit])

        @pl.when((s == 0) | (s == steps - 1))
        def _():
            @pl.when(s == 0)
            def _():
                x_copy(0).wait()
                for m in range(1, tiles):
                    x_copy(m).start()

            @pl.loop(0, tiles)
            def _(m):
                @pl.when((s == 0) & (m > 0))
                def _():
                    x_copy(m).wait()

                compute(m, span(m, tile), act_v.at[0])

                @pl.when(s == steps - 1)
                def _():
                    @pl.loop(0, tile // 96)
                    def _(i):
                        at = span(m * (tile // 96) + i, 96)
                        x_v[at, :] = acc_v[at, :].astype(BF16)

                    out_copy(m).start()

        @pl.when((s > 0) & (s < steps - 1))
        def _():
            for m in range(tiles):
                compute(m, pl.ds(m * tile, tile), act_v.at[m % 2])

    for j in (pieces - 2, pieces - 1):
        wait_recv(core_b(j))
    wait_send(own_copies())

    @pl.loop(0, pieces)
    def _(j):
        for copies in (chip_copies(j), group_a(j), core_a(j), core_b(j)):
            wait_send(copies)

    for m in range(tiles):
        out_copy(m).wait()


def mlp(x2, w_gate, w_up, w_down):
    rows, width = x2.shape
    ff = w_gate.shape[1]
    unit = 512
    tile = rows // 6
    far = ff // 2 // unit
    pieces = 2 * far
    shapes = [(rows, width), (width, ff), (width, ff), (ff, width), (4, far, width, unit), (4, far, width, unit), (4, far, unit, width)]
    any_spec = pl.BlockSpec(memory_space=pl.ANY)
    dma = pltpu.SemaphoreType.DMA
    out = pl.pallas_call(
        mlp_kernel,
        in_specs=[any_spec] * 4,
        out_specs=[any_spec] * 7,
        out_shape=[jax.ShapeDtypeStruct(s, BF16) for s in shapes],
        scratch_shapes=[
            pltpu.VMEM((rows, width), BF16),
            pltpu.VMEM((rows, width), F32),
            pltpu.VMEM((2, tile, unit), BF16),
            pltpu.VMEM((2, width, unit), BF16),
            pltpu.VMEM((2, width, unit), BF16),
            pltpu.VMEM((2, unit, width), BF16),
            dma((2, 3)),
            dma((rows // tile,)),
            dma((rows // tile,)),
            dma((3,)),
            dma((3,)),
        ]
        + [dma((pieces, 3))] * 8,
        compiler_params=pltpu.CompilerParams(vmem_limit_bytes=VMEM_LIMIT, collective_id=0, has_side_effects=True),
        cost_estimate=pl.CostEstimate(flops=2 * rows * width * ff * 3 * 4, bytes_accessed=4 * 3 * width * ff * 2, transcendentals=0),
        name="mlp",
    )(x2, w_gate, w_up, w_down)
    return out[0], out[4:]


def last_kernel(x_ref, part_ref, h_ref, wg_ref, wu_ref, wd_ref, key_hbm, value_hbm, out_ref, key_out, value_out, act_v, cache_v, sem):
    i = pl.program_id(0)
    pairs = ((key_hbm, key_out), (value_hbm, value_out))
    loads = [pltpu.make_async_copy(src, cache_v.at[n], sem.at[n]) for n, (src, _) in enumerate(pairs)]
    stores = [pltpu.make_async_copy(cache_v.at[n], dst, sem.at[n]) for n, (_, dst) in enumerate(pairs)]

    @pl.when(i == 0)
    def _():
        start(loads)

    @pl.when(i == 1)
    def _():
        for load, store in zip(loads, stores):
            load.wait()
            store.start()

    expand(x_ref, wg_ref.at[0, 0], wu_ref.at[0, 0], act_v)
    block = 512
    for n in range(0, out_ref.shape[1], block):
        at = slice(n, n + block)
        total = part_ref[:, at].astype(F32) + dot(act_v[...], wd_ref[0, 0, :, at])
        out_ref[:, at] = (h_ref[:, at].astype(F32) + total.astype(BF16).astype(F32)).astype(BF16)

    @pl.when(i == pl.num_programs(0) - 1)
    def _():
        for store in stores:
            store.wait()


def finish(x2, part, h1, far_weights, key, value):
    rows, width = x2.shape
    tile = rows // 6
    groups, per_group = far_weights[0].shape[:2]
    row_block = pl.BlockSpec((tile, width), lambda i: (i, 0))
    any_spec = pl.BlockSpec(memory_space=pl.ANY)

    def weight_block(w):
        return pl.BlockSpec((1, 1) + w.shape[2:], lambda i: (groups - 1, per_group - 1, 0, 0), pipeline_mode=pl.Buffered(1))

    unit = far_weights[0].shape[3]
    shape = jax.ShapeDtypeStruct
    return pl.pallas_call(
        last_kernel,
        grid=(rows // tile,),
        in_specs=[row_block] * 3 + [weight_block(w) for w in far_weights] + [any_spec] * 2,
        out_specs=[row_block, any_spec, any_spec],
        out_shape=[shape(x2.shape, BF16), shape(key.shape, BF16), shape(value.shape, BF16)],
        scratch_shapes=[pltpu.VMEM((tile, unit), BF16), pltpu.VMEM((2,) + key.shape, BF16), pltpu.SemaphoreType.DMA((2,))],
        compiler_params=pltpu.CompilerParams(dimension_semantics=("arbitrary",), vmem_limit_bytes=60 << 20),
        cost_estimate=pl.CostEstimate(flops=6 * rows * width * unit, bytes_accessed=8 * rows * width, transcendentals=0),
        name="finish",
    )(x2, part, h1, *far_weights, key, value)


def solution(mesh):
    tp_size = mesh.shape["tp"]
    row_spec = P("dp", "tp", None)
    arg_specs = (row_spec, P("dp"), P("dp"), P(), P(None, "tp"), P(), P(), P("tp", None), P(), P(None, "tp"), P(None, "tp"), P("tp", None))

    def local_layer(hidden, prefix_len, valid_len, norm_attn, w_query, w_key, w_value, w_out, norm_mlp, w_gate, w_up, w_down):
        h1, x2, key, value = attention(hidden, prefix_len, valid_len, norm_attn, norm_mlp, w_query, w_key, w_value, w_out, tp_size)
        flat = (-1, hidden.shape[-1])
        x2 = x2.reshape(flat)
        part, far_weights = mlp(x2, w_gate, w_up, w_down)
        out, key, value = finish(x2, part, h1.reshape(flat), far_weights, key, value)
        return out.reshape(hidden.shape), key, value

    return jax.shard_map(local_layer, mesh=mesh, in_specs=arg_specs, out_specs=(row_spec, row_spec, row_spec), check_vma=False)
```
